32 devices in a mesh: sta: 16 (over z, x, core), tpl: 2 (over y).
Axes of the slice: x: 2, y: 2, z: 4, core: 2. Of those that a mesh axis runs over, the one named last changes fastest.
Arguments:
- waveform: bfloat16 [16, 3, 4279], P('sta'), may hold values from -150 to 150
- templates: bfloat16 [128, 16, 1536], P('tpl', 'sta'), may hold values from -6 to 6
- lags: int32 [128, 16], P('tpl', 'sta'), may hold values from 0 to 3000
- present: int32 [128, 16], P('tpl', 'sta'), may hold values 0 or 1
Outputs:
- score: float32 [768, 128], P('sta', 'tpl')
- scale_mad: float32 [128], P('tpl')
- peak: float32 [768], P('sta')
The draws below stay inside these ranges and needn't reach their ends.
All inputs are finite; a program needn't handle non-finite values. No bound on the sum of `present` on one device may be relied on, other than what follows from the above.
Results may differ from the reference program's by a relative error of at most 0.0003.
Values may be sent and summed in bfloat16 or wider, within the bound.
A program may use at most 64 MiB of HBM per device.

```python
import jax
import jax.numpy as jnp
from jax import lax

LEN = 512
CHANS = 3
LAG = 3000
BINS = 1024
STATIONS = 16
TEMPLATES = 128
TOUT = 768
SAMPLES = 4279


def draw_waveform(key, part):
    key_noise = jax.random.fold_in(key, 11)
    key_scale = jax.random.fold_in(key, 12)
    timeline = jnp.arange(SAMPLES, dtype=jnp.float32) / SAMPLES
    envelope = jnp.exp(jnp.log(3.0) * timeline)
    noise = jnp.clip(jax.random.normal(key_noise, (STATIONS, 3, SAMPLES), jnp.float32), -5.0, 5.0)
    scales = jnp.exp(jax.random.uniform(key_scale, (STATIONS, 1, 1), jnp.float32, 0.0, jnp.log(10.0)))
    return (noise * scales * envelope).astype(jnp.bfloat16)


def touch_ends(drawn, own_key, smallest, top_value):
    longest = drawn.shape.index(max(drawn.shape))
    spots = []
    for shift in (0, 1):
        where = [jax.random.randint(jax.random.fold_in(own_key, axis), (), 0, length) for axis, length in enumerate(drawn.shape)]
        where[longest] = (where[longest] + shift) % drawn.shape[longest]
        spots.append(tuple(where))
    return drawn.at[spots[0]].set(smallest).at[spots[1]].set(top_value)


def shard_levels(own_key, extent, shards, least, high):
    loudness, own = 1.0, jax.random.fold_in(own_key, 6)
    for axis_at, blocks in shards:
        draws = jnp.exp(jax.random.uniform(jax.random.fold_in(own, axis_at), (blocks,), jnp.float32, least / len(shards), high / len(shards)))
        loudness = loudness * jnp.repeat(draws, extent[axis_at] // blocks).reshape([-1 if axis == axis_at else 1 for axis in range(len(extent))])
    return loudness


def normal_values(own_key, extent, scale, most, pieces=(), held_as=jnp.bfloat16):
    values = scale * jax.random.normal(own_key, extent, jnp.float32)
    if pieces:
        values = values * shard_levels(own_key, extent, pieces, -0.22, 0.18)
    return jnp.clip(values, -most, most).astype(held_as)


def setup_inputs(seed: int = 0) -> dict:
    streams_of = jax.random.split(jax.random.key(seed), 5)
    waveform = draw_waveform(jax.random.fold_in(streams_of[4], 71), 0)
    templates = normal_values(streams_of[1], (TEMPLATES, STATIONS, CHANS * LEN), 1.0, 6.0, ((0, 2), (1, 16)))
    lags = touch_ends(jax.random.randint(streams_of[2], (TEMPLATES, STATIONS), 0, LAG + 1), jax.random.fold_in(streams_of[2], 1), 0, LAG).astype(jnp.int32)
    present = touch_ends((jax.random.randint(streams_of[3], (TEMPLATES, STATIONS), 0, 4) < 3).astype(jnp.int32), jax.random.fold_in(streams_of[3], 1), 0, 1)
    return dict(waveform=waveform, templates=templates, lags=lags, present=present)


def toeplitz_rows(record, length, columns):
    count = record.shape[1]
    chans = record.shape[0]
    tiled = jnp.broadcast_to(record[:, None, :], (chans, length + 1, count))
    tiled = tiled.reshape(chans, (length + 1) * count)[:, :length * (count + 1)]
    tiled = tiled.reshape(chans, length, count + 1)[:, :, :columns]
    return tiled.reshape(chans * length, columns)

def shift_rows(block, offsets, count):
    return jax.vmap(lambda row, offset: lax.dynamic_slice_in_dim(row, offset, count))(block, offsets.astype(jnp.int32))

def hat_counts(values, nbins):
    width = 512.0 / nbins
    ncols = values.shape[1]
    position = jnp.clip(jnp.abs(values) / width - 0.5, 0.0, nbins - 1.0)
    lower = jnp.minimum(jnp.floor(position), nbins - 2.0)
    weight = position - lower
    index = lower.astype(jnp.int32) + nbins * jnp.arange(ncols, dtype=jnp.int32)[None, :]
    flat_index = index.reshape(-1)
    flat_weight = weight.reshape(-1)
    counts = jax.ops.segment_sum(1.0 - flat_weight, flat_index, num_segments=ncols * nbins)
    counts = counts + jax.ops.segment_sum(flat_weight, flat_index + 1, num_segments=ncols * nbins)
    return counts.reshape(ncols, nbins)

def median_abs(counts, halfway):
    width = 512.0 / counts.shape[1]
    running = jnp.cumsum(counts, axis=1)
    earlier = running - counts
    share = jnp.clip((halfway - earlier) / jnp.maximum(counts, 1.0), 0.0, 1.0)
    return width * lax.optimization_barrier(jnp.sum(share, axis=1))

def reference(waveform, templates, lags, present):
    total = TOUT
    span = TOUT + LAG
    tnorm = jnp.sqrt(lax.optimization_barrier(jnp.sum(templates.astype(jnp.float32) ** 2, axis=2)) + 1e-06)

    def station(stack, items):
        record, pattern, offsets, member, scaling = items
        columns = toeplitz_rows(record, LEN, span)
        corr = jnp.dot(pattern, columns, preferred_element_type=jnp.float32) / scaling[:, None]
        moved = shift_rows(corr, offsets, total) * member[:, None].astype(jnp.float32)
        return (stack + moved, None)
    start = jnp.zeros((templates.shape[0], total), jnp.float32)
    stack, unused = lax.scan(station, start, (waveform, jnp.swapaxes(templates, 0, 1), lags.T, present.T, tnorm.T))
    stack = stack.T
    counts = hat_counts(stack, BINS)
    median = median_abs(counts, 0.5 * total)
    scale_mad = 1.4826 * median
    score = stack / scale_mad[None, :]
    peak = lax.optimization_barrier(jnp.max(score, axis=1))
    return (score, scale_mad, peak)
```

```python
import functools

import jax
import jax.numpy as jnp
from jax import lax
from jax.experimental import pallas as pl
from jax.experimental.pallas import tpu as pltpu
from jax.sharding import PartitionSpec as P

LEN = 512
LAG = 3000
BINS = 1024
TOUT_DEV = 48
LANES = 128
MESH = pl.DeviceIdType.MESH


def ceil_to(value, step):
    return -(-value // step) * step


def build_hankel(wave_ref, record, hankel):
    chans, samples = wave_ref.shape
    span = hankel.shape[2]
    record[...] = jnp.zeros_like(record)
    record[:, :samples] = wave_ref[...].astype(jnp.float32)
    piece = 8 * LANES
    for start in range(0, span, piece):
        size = min(piece, span - start)
        wide = size + LANES
        row = lax.broadcasted_iota(jnp.int32, (8, wide), 0)
        for c in range(chans):
            base = jnp.broadcast_to(record[c : c + 1, start : start + wide], (8, wide))
            for bit in (1, 2, 4):
                base = jnp.where((row & bit) != 0, pltpu.roll(base, wide - bit, 1), base)
            both = jnp.concatenate([base, pltpu.roll(base, wide - 8, 1)], axis=0).astype(jnp.bfloat16)
            for g in range(LANES // 16):
                hankel[c, 16 * g : 16 * g + 16, start : start + size] = both[:, 16 * g : 16 * g + size]


def correlate_blocks(blocks, stride, pattern_ref, hankel, corr):
    chans = hankel.shape[0]
    rows = pattern_ref.shape[0]
    pattern = pattern_ref[...]
    wide = pattern.astype(jnp.float32)
    factor = 1.0 / jnp.sqrt(jnp.sum(wide * wide, axis=1, keepdims=True) + 1e-06)
    depth = 2 * LANES
    halves = []
    for h in range(LEN // depth):
        halves.append(jnp.concatenate([pattern[:, c * LEN + h * depth : c * LEN + (h + 1) * depth] for c in range(chans)], axis=1))
    stacked = jnp.concatenate(halves, axis=0)
    pending = None
    for b in range(blocks + 1):
        begin = depth * b
        parts = []
        for c in range(chans):
            for q in range(2):
                parts.append(hankel[c, :, begin + LANES * q : begin + LANES * q + depth])
        columns = jnp.concatenate(parts, axis=0)
        result = jnp.dot(stacked, columns, preferred_element_type=jnp.float32)
        if b:
            total = (pending + result[rows:]) * factor
            corr[pl.ds(2 * b - 2, rows, stride=stride), :] = total[:, :LANES]
            corr[pl.ds(2 * b - 1, rows, stride=stride), :] = total[:, LANES:]
        pending = result[:rows]


def deviation_scale(stack, groups, total):
    width = 512.0 / BINS
    count = stack.shape[0] // groups
    position = jnp.clip(jnp.abs(stack) / width - 0.5, 0.0, BINS - 1.0)
    lower = jnp.minimum(jnp.floor(position), BINS - 2.0)
    coarse = jnp.floor(lower * 0.125)
    fine = position - 8.0 * coarse
    sub = lax.broadcasted_iota(jnp.int32, (LANES, LANES), 0).astype(jnp.float32)
    few = lax.broadcasted_iota(jnp.int32, (16, LANES), 0).astype(jnp.float32)
    tables = []
    for t in range(groups):
        hots, weights = [], []
        for a in range(count):
            r = t * count + a
            hots.append((coarse[r : r + 1, :] == sub).astype(jnp.float32).astype(jnp.bfloat16))
            hat = jnp.maximum(1.0 - jnp.abs(fine[r : r + 1, :] - few), 0.0)
            first = hat.astype(jnp.bfloat16)
            left = hat - first.astype(jnp.float32)
            second = left.astype(jnp.bfloat16)
            third = (left - second.astype(jnp.float32)).astype(jnp.bfloat16)
            weights.append(jnp.concatenate([first, second, third], axis=0))
        hot = jnp.concatenate(hots, axis=1)
        weight = jnp.concatenate(weights, axis=1)
        found = lax.dot_general(weight, hot, (((1,), (1,)), ((), ())), preferred_element_type=jnp.float32)
        found = found[:16] + found[16:32] + found[32:48]
        tables.append(found[:8] + pltpu.roll(found[8:], 1, 1))
    counts = jnp.concatenate(tables, axis=0)
    row = lax.broadcasted_iota(jnp.int32, counts.shape, 0) & 7
    running = counts
    for step in (1, 2, 4):
        running = running + jnp.where(row >= step, pltpu.roll(running, step, 0), 0.0)
    sums = [jnp.broadcast_to(jnp.sum(t, axis=0, keepdims=True), (8, LANES)) for t in tables]
    sums = jnp.concatenate(sums, axis=0)
    upper = (
        lax.broadcasted_iota(jnp.int32, (LANES, LANES), 0) < lax.broadcasted_iota(jnp.int32, (LANES, LANES), 1)
    ).astype(jnp.float32)
    prior = jnp.dot(sums, upper, precision=lax.Precision.HIGHEST, preferred_element_type=jnp.float32)
    earlier = prior + (running - counts)
    share = jnp.clip((0.5 * total - earlier) / jnp.maximum(counts, 1.0), 0.0, 1.0)
    scales = []
    for t in range(groups):
        part = jnp.sum(share[8 * t : 8 * t + 8], axis=0, keepdims=True)
        scales.append(1.4826 * (width * jnp.sum(part, axis=1, keepdims=True)))
    return scales


LEVELS = 32600.0
ROUNDER = 12582912.0
CODE_STEP = 64.0


def encode(pieces, target, slot):
    half = len(pieces) // 2
    rows = pieces[0].shape[0]
    most = jnp.abs(pieces[0])
    for piece in pieces[1:]:
        most = jnp.maximum(most, jnp.abs(piece))
    most = jnp.maximum(jnp.max(most, axis=0, keepdims=True), 1e-30)
    code = jnp.floor(jnp.log2(most) * CODE_STEP) + 1.0
    inverse = LEVELS * jnp.exp2(code * (-1.0 / CODE_STEP))
    for p in range(half):
        high = (pieces[p] * inverse + ROUNDER).astype(jnp.int32)
        low = (pieces[p + half] * inverse + ROUNDER).astype(jnp.int32)
        target[slot, p * rows : (p + 1) * rows, :] = (high << 16) | (low & 65535)
    target[slot, half * rows : half * rows + 1, :] = code.astype(jnp.int32)


def decode(source, slot, half, rows):
    code = source[slot, half * rows : half * rows + 1, :].astype(jnp.float32)
    scale = jnp.exp2(code * (1.0 / CODE_STEP)) * (1.0 / LEVELS)
    highs, lows = [], []
    for p in range(half):
        word = source[slot, p * rows : (p + 1) * rows, :]
        highs.append((word >> 16).astype(jnp.float32) * scale)
        lows.append(((word << 16) >> 16).astype(jnp.float32) * scale)
    return highs + lows


def stack_kernel(n, m, own, blocks, stride, lags_hbm, present_hbm, wave_hbm, pattern_hbm, out_ref, lags_ref, present_ref, wave_ref, pattern_ref, load_sem, record, hankel, corr, packed, recv1, scored, send2, recv2, send3, recv3, send_sem, recv1_sem, recv2_sem, recv3_sem):
    me, group = lax.axis_index("sta"), lax.axis_index("tpl")
    groups = send2.shape[1]
    rows = pattern_ref.shape[0]
    count = n * own // LANES
    chunk = groups * count
    pieces = max(groups, 2)
    split = pieces // groups
    piece_rows = chunk // pieces
    half = pieces // 2

    def peer(d):
        return me ^ d

    def fellow(e):
        return lax.rem(group + e, m)

    loads = [
        pltpu.make_async_copy(source, target, load_sem.at[k])
        for k, (source, target) in enumerate(
            ((wave_hbm, wave_ref), (pattern_hbm, pattern_ref), (lags_hbm, lags_ref), (present_hbm, present_ref))
        )
    ]
    for load in loads:
        load.start()

    barrier = pltpu.get_barrier_semaphore()
    for e in range(m):

        def greet(d, carry):
            pl.semaphore_signal(barrier, inc=1, device_id={"sta": peer(d), "tpl": fellow(e)}, device_id_type=MESH)
            return carry

        lax.fori_loop(0 if e else 1, n, greet, 0)

    bands = []
    low = 1
    while low < n:
        bands.append((low, min(2 * low, n)))
        low *= 2
    if len(bands) > 2:
        bands[:2] = [(1, bands[1][1])]

    def copy1(d, band):
        return pltpu.make_async_remote_copy(
            src_ref=packed.at[d],
            dst_ref=recv1.at[d],
            send_sem=send_sem.at[0],
            recv_sem=recv1_sem.at[band],
            device_id={"sta": peer(d), "tpl": group},
            device_id_type=MESH,
        )

    def all1(low, high, band):
        return pltpu.make_async_remote_copy(
            src_ref=packed.at[pl.ds(low, high - low)],
            dst_ref=recv1.at[pl.ds(low, high - low)],
            send_sem=send_sem.at[0],
            recv_sem=recv1_sem.at[band],
            device_id={"sta": peer(1), "tpl": group},
            device_id_type=MESH,
        )

    def copy2(d):
        return pltpu.make_async_remote_copy(
            src_ref=send2.at[peer(d)],
            dst_ref=recv2.at[me],
            send_sem=send_sem.at[1],
            recv_sem=recv2_sem,
            device_id={"sta": peer(d), "tpl": group},
            device_id_type=MESH,
        )

    def all2():
        return pltpu.make_async_remote_copy(
            src_ref=send2.at[pl.ds(1, n - 1)],
            dst_ref=recv2.at[pl.ds(1, n - 1)],
            send_sem=send_sem.at[1],
            recv_sem=recv2_sem,
            device_id={"sta": peer(1), "tpl": group},
            device_id_type=MESH,
        )

    def copy3(e, d):
        return pltpu.make_async_remote_copy(
            src_ref=send3.at[peer(d)],
            dst_ref=recv3.at[e - 1, d],
            send_sem=send_sem.at[2],
            recv_sem=recv3_sem,
            device_id={"sta": peer(d), "tpl": fellow(e)},
            device_id_type=MESH,
        )

    def all3():
        return pltpu.make_async_remote_copy(
            src_ref=recv3,
            dst_ref=recv3,
            send_sem=send_sem.at[2],
            recv_sem=recv3_sem,
            device_id={"sta": peer(1), "tpl": group},
            device_id_type=MESH,
        )

    loads[0].wait()
    build_hankel(wave_ref, record, hankel)
    loads[1].wait()
    correlate_blocks(blocks, stride, pattern_ref, hankel, corr)

    loads[2].wait()
    loads[3].wait()
    lane = lax.broadcasted_iota(jnp.int32, (piece_rows, LANES), 1)

    def shifted(d):
        found = []
        for p in range(pieces):
            t = peer(d) * groups + p // split
            lag = lags_ref[t]
            begin = t * stride + (lag >> 7) + (p % split) * piece_rows
            rest = lag & (LANES - 1)
            near = corr[pl.ds(begin, piece_rows), :]
            after = corr[pl.ds(begin + 1, piece_rows), :]
            joined = pltpu.roll(jnp.where(lane >= rest, near, after), (LANES - rest) & (LANES - 1), 1)
            found.append(joined * present_ref[t].astype(jnp.float32))
        return found

    batch = max(n // 4, 1)
    order = list(range(n - 1, 0, -1))
    for begin in range(0, n - 1, batch):
        for d in order[begin : begin + batch]:
            encode(shifted(d), packed, d)
        if begin == 0:
            pl.semaphore_wait(barrier, n * m - 1)
        for d in order[begin : begin + batch]:
            band = next(k for k, (a, b) in enumerate(bands) if a <= d < b)
            copy1(d, band).start()
    total = shifted(0)
    for k, (low, high) in enumerate(bands):
        all1(low, high, k).wait_recv()
        for d in range(low, high):
            total = [a + b for a, b in zip(total, decode(recv1, d, half, piece_rows))]
    stack = jnp.concatenate(total, axis=0)
    scales = deviation_scale(stack, groups, n * own)
    scored[chunk:, :] = jnp.zeros((8, LANES), jnp.float32)
    for t in range(groups):
        scored[t * count : (t + 1) * count, :] = stack[t * count : (t + 1) * count, :] / scales[t]
    scale = jnp.concatenate(scales, axis=0)
    lane = lax.broadcasted_iota(jnp.int32, (groups, LANES), 1)
    for j in range(n):
        begin, rest = divmod(own * j, LANES)
        near = scored[pl.ds(begin, groups, stride=count), :]
        if rest:
            after = scored[pl.ds(begin + 1, groups, stride=count), :]
            near = pltpu.roll(jnp.where(lane >= rest, near, after), LANES - rest, 1)
        send2[j] = jnp.where(lane < own, near, scale)
        send3[j] = jnp.max(near, axis=0, keepdims=True)

    if m == 2:
        for d in range(n - 1, -1, -1):
            copy3(1, d).start()
    else:
        for e in range(1, m):

            def start3(d, carry):
                copy3(e, d).start()
                return carry

            lax.fori_loop(0, n, start3, 0)
    for d in range(n - 1, 0, -1):
        copy2(d).start()
    recv2[me] = send2[me]
    all1(1, n, 0).wait_send()

    all2().wait_recv()
    top = recv2[0]
    out_ref[:groups, :] = top
    for i in range(1, n):
        out_ref[i * groups : (i + 1) * groups, :] = recv2[i]
        top = jnp.maximum(top, recv2[i])
    top = jnp.max(top, axis=0, keepdims=True)
    if m > 1:
        all3().wait_recv()
        for e in range(m - 1):
            top = jnp.maximum(top, jnp.max(recv3[e], axis=0))
    lane = lax.broadcasted_iota(jnp.int32, (8, LANES), 1)
    moved_top = jnp.broadcast_to(pltpu.roll(top, LANES // 2, 1), (8, LANES))
    out_ref[:8, :] = jnp.where(lane < LANES // 2, out_ref[:8, :], moved_top)

    all2().wait_send()
    if m > 1:
        all3().wait_send()


def stack_and_score(wave, pattern, lags, present, n, m):
    chans, samples = wave.shape
    rows = pattern.shape[0]
    total = TOUT_DEV * n
    blocks = -(-(total + LAG) // (2 * LANES))
    span = 2 * LANES * (blocks + 1) + LANES
    padded = ceil_to(max(span + LANES, samples), LANES)
    count = total // LANES
    stride = max(2 * blocks, LAG // LANES + count + 2) | 1
    groups = rows // n
    chunk = groups * count
    words = chunk // 2 + 1
    vmem = pl.BlockSpec(memory_space=pltpu.VMEM)
    return pl.pallas_call(
        functools.partial(stack_kernel, n, m, TOUT_DEV, blocks, stride),
        out_shape=jax.ShapeDtypeStruct((rows, LANES), jnp.float32),
        in_specs=[pl.BlockSpec(memory_space=pl.ANY)] * 4,
        out_specs=vmem,
        scratch_shapes=[
            pltpu.SMEM(lags.shape, lags.dtype),
            pltpu.SMEM(present.shape, present.dtype),
            pltpu.VMEM(wave.shape, wave.dtype),
            pltpu.VMEM(pattern.shape, pattern.dtype),
            pltpu.SemaphoreType.DMA((4,)),
            pltpu.VMEM((chans, padded), jnp.float32),
            pltpu.VMEM((chans, LANES, span), jnp.bfloat16),
            pltpu.VMEM((rows * stride, LANES), jnp.float32),
            pltpu.VMEM((n, words, LANES), jnp.int32),
            pltpu.VMEM((n, words, LANES), jnp.int32),
            pltpu.VMEM((chunk + 8, LANES), jnp.float32),
            pltpu.VMEM((n, groups, LANES), jnp.float32),
            pltpu.VMEM((n, groups, LANES), jnp.float32),
            pltpu.VMEM((n, 1, LANES), jnp.float32),
            pltpu.VMEM((max(m - 1, 1), n, 1, LANES), jnp.float32),
            pltpu.SemaphoreType.DMA((3,)),
            pltpu.SemaphoreType.DMA((max((n - 1).bit_length() - 1, 1),)),
            pltpu.SemaphoreType.DMA,
            pltpu.SemaphoreType.DMA,
        ],
        compiler_params=pltpu.CompilerParams(collective_id=0, has_side_effects=True),
    )(lags, present, wave, pattern)


def finish_kernel(grid_ref, score_ref, scale_ref, peak_ref):
    own, rows = score_ref.shape
    turned = grid_ref[...].T
    score_ref[...] = turned[:own, :]
    scale_ref[...] = turned[own, :]
    peak_ref[...] = grid_ref[0, LANES // 2 : LANES // 2 + own]


def on_device(waveform, templates, lags, present):
    n, m = lax.axis_size("sta"), lax.axis_size("tpl")
    rows = templates.shape[0]
    grid = stack_and_score(waveform[0], templates[:, 0, :], lags[:, 0], present[:, 0], n, m)
    return pl.pallas_call(
        finish_kernel,
        out_shape=(
            jax.ShapeDtypeStruct((TOUT_DEV, rows), jnp.float32),
            jax.ShapeDtypeStruct((rows,), jnp.float32),
            jax.ShapeDtypeStruct((TOUT_DEV,), jnp.float32),
        ),
    )(grid)


def solution(mesh):
    placed = (P("sta", None, None), P("tpl", "sta", None), P("tpl", "sta"), P("tpl", "sta"))
    return jax.shard_map(
        on_device,
        mesh=mesh,
        in_specs=placed,
        out_specs=(P("sta", "tpl"), P("tpl"), P("sta")),
        check_vma=False,
    )
```

```python
import functools

import jax
import jax.numpy as jnp
from jax import lax
from jax.experimental import pallas as pl
from jax.experimental.pallas import tpu as pltpu
from jax.sharding import PartitionSpec as P

LEN = 512
LAG = 3000
BINS = 1024
TOUT_DEV = 48
LANES = 128
VMEM_LIMIT = 16 * 1024 * 1024
MESH = pl.DeviceIdType.MESH


def ceil_to(value, step):
    return -(-value // step) * step


def build_hankel(record, hankel, first, last):
    back = lax.broadcasted_iota(jnp.int32, (8, LANES), 1) - lax.broadcasted_iota(jnp.int32, (8, LANES), 0)

    def turned(c, j, a):
        line = jnp.broadcast_to(record[c : c + 1, j * LANES : (j + 1) * LANES], (8, LANES))
        return pltpu.roll(line, LANES - 7 - 8 * a, 1, stride=1, stride_axis=0)

    for c in range(hankel.shape[0]):
        for g in range(LANES // 16):
            halves = []
            for a in (2 * g, 2 * g + 1):
                now = turned(c, first, a)
                pieces = []
                for j in range(first, last):
                    later = turned(c, j + 1, a)
                    pieces.append(jnp.where(back < LANES - 7 - 8 * a, now, later))
                    now = later
                halves.append(jnp.concatenate(pieces, axis=1))
            hankel[c, 16 * g : 16 * g + 16, first * LANES : last * LANES] = jnp.concatenate(halves, axis=0).astype(jnp.bfloat16)


def reverse_eights(pattern):
    rows, width = pattern.shape
    source = lax.broadcasted_iota(jnp.int32, (LANES, LANES), 0)
    target = lax.broadcasted_iota(jnp.int32, (LANES, LANES), 1)
    swap = (source == (target ^ 7)).astype(jnp.float32).astype(jnp.bfloat16)
    chunks = jnp.concatenate([pattern[:, k * LANES : (k + 1) * LANES] for k in range(width // LANES)], axis=0)
    turned = jnp.dot(chunks, swap, preferred_element_type=jnp.float32).astype(jnp.bfloat16)
    return [turned[k * rows : (k + 1) * rows] for k in range(width // LANES)]


def correlate(blocks, stride, wave_ref, pattern_ref, record, hankel, corr):
    chans, samples = wave_ref.shape
    rows = pattern_ref.shape[0]
    span = hankel.shape[2]
    record[...] = jnp.zeros_like(record)
    record[:, :samples] = wave_ref[...].astype(jnp.float32)
    pattern = pattern_ref[...]
    wide = pattern.astype(jnp.float32)
    factor = 1.0 / jnp.sqrt(jnp.sum(wide * wide, axis=1, keepdims=True) + 1e-06)
    depth = 2 * LANES
    chunks = reverse_eights(pattern)
    per = LEN // LANES
    stacked = []
    for c in range(chans):
        halves = [jnp.concatenate([chunks[c * per + 2 * h + q] for q in range(2)], axis=1) for h in range(LEN // depth)]
        stacked.append(jnp.concatenate(halves, axis=0))
    built = 0
    pending = None
    for first in range(0, blocks + 1, 2):
        begin = depth * first
        width = depth * min(2, blocks + 1 - first)
        need = begin + width + LANES
        build_hankel(record, hankel, built // LANES, need // LANES)
        built = need
        for b in range(first, first + width // depth):
            piece = None
            for c in range(chans):
                start = depth * b
                columns = jnp.concatenate([hankel[c, :, start + LANES * q : start + LANES * q + depth] for q in range(2)], axis=0)
                part = jnp.dot(stacked[c], columns, preferred_element_type=jnp.float32)
                piece = part if piece is None else piece + part
            if b:
                total = (pending + piece[rows:]) * factor
                corr[pl.ds(2 * b - 2, rows, stride=stride), :] = total[:, :LANES]
                corr[pl.ds(2 * b - 1, rows, stride=stride), :] = total[:, LANES:]
            pending = piece[:rows]


def deviation_scale(stack, groups, total):
    width = 512.0 / BINS
    count = stack.shape[0] // groups
    position = jnp.clip(jnp.abs(stack) / width - 0.5, 0.0, BINS - 1.0)
    lower = jnp.minimum(jnp.floor(position), BINS - 2.0)
    coarse = jnp.floor(lower * 0.125)
    fine = position - 8.0 * coarse
    sub = lax.broadcasted_iota(jnp.int32, (LANES, LANES), 0).astype(jnp.float32)
    few = lax.broadcasted_iota(jnp.int32, (16, LANES), 0).astype(jnp.float32)
    tables = []
    for t in range(groups):
        hots, weights = [], []
        for a in range(count):
            r = t * count + a
            hots.append((coarse[r : r + 1, :] == sub).astype(jnp.float32).astype(jnp.bfloat16))
            hat = jnp.maximum(1.0 - jnp.abs(fine[r : r + 1, :] - few), 0.0)
            first = hat.astype(jnp.bfloat16)
            left = hat - first.astype(jnp.float32)
            second = left.astype(jnp.bfloat16)
            third = (left - second.astype(jnp.float32)).astype(jnp.bfloat16)
            weights.append(jnp.concatenate([first, second, third], axis=0))
        hot = jnp.concatenate(hots, axis=1)
        weight = jnp.concatenate(weights, axis=1)
        found = lax.dot_general(weight, hot, (((1,), (1,)), ((), ())), preferred_element_type=jnp.float32)
        found = found[:16] + found[16:32] + found[32:48]
        tables.append(found[:8] + pltpu.roll(found[8:], 1, 1))
    counts = jnp.concatenate(tables, axis=0)
    row = lax.broadcasted_iota(jnp.int32, counts.shape, 0) & 7
    running = counts
    for step in (1, 2, 4):
        running = running + jnp.where(row >= step, pltpu.roll(running, step, 0), 0.0)
    sums = [jnp.broadcast_to(jnp.sum(t, axis=0, keepdims=True), (8, LANES)) for t in tables]
    sums = jnp.concatenate(sums, axis=0)
    upper = (
        lax.broadcasted_iota(jnp.int32, (LANES, LANES), 0) < lax.broadcasted_iota(jnp.int32, (LANES, LANES), 1)
    ).astype(jnp.float32)
    prior = jnp.dot(sums, upper, precision=lax.Precision.HIGHEST, preferred_element_type=jnp.float32)
    earlier = prior + (running - counts)
    share = jnp.clip((0.5 * total - earlier) / jnp.maximum(counts, 1.0), 0.0, 1.0)
    scales = []
    for t in range(groups):
        part = jnp.sum(share[8 * t : 8 * t + 8], axis=0, keepdims=True)
        scales.append(1.4826 * (width * jnp.sum(part, axis=1, keepdims=True)))
    return scales


LEVELS = 32600.0
ROUNDER = 12582912.0
CODE_STEP = 64.0


def encode(pieces, target, slot):
    half = len(pieces) // 2
    rows = pieces[0].shape[0]
    most = jnp.abs(pieces[0])
    for piece in pieces[1:]:
        most = jnp.maximum(most, jnp.abs(piece))
    most = jnp.maximum(jnp.max(most, axis=0, keepdims=True), 1e-30)
    code = jnp.floor(jnp.log2(most) * CODE_STEP) + 1.0
    inverse = LEVELS * jnp.exp2(code * (-1.0 / CODE_STEP))
    for p in range(half):
        high = (pieces[p] * inverse + ROUNDER).astype(jnp.int32)
        low = (pieces[p + half] * inverse + ROUNDER).astype(jnp.int32)
        target[slot, p * rows : (p + 1) * rows, :] = (high << 16) | (low & 65535)
    target[slot, half * rows : half * rows + 1, :] = code.astype(jnp.int32)


def decode(source, slot, half, rows):
    code = source[slot, half * rows : half * rows + 1, :].astype(jnp.float32)
    scale = jnp.exp2(code * (1.0 / CODE_STEP)) * (1.0 / LEVELS)
    highs, lows = [], []
    for p in range(half):
        word = source[slot, p * rows : (p + 1) * rows, :]
        highs.append((word >> 16).astype(jnp.float32) * scale)
        lows.append(((word << 16) >> 16).astype(jnp.float32) * scale)
    return highs + lows


def stack_kernel(n, m, own, blocks, stride, lags_hbm, present_hbm, wave_hbm, pattern_hbm, out_ref, lags_ref, present_ref, wave_ref, pattern_ref, load_sem, record, hankel, corr, packed, recv1, scored, send2, recv2, send3, recv3, send_sem, recv1_sem, recv2_sem, recv3_sem):
    me, group = lax.axis_index("sta"), lax.axis_index("tpl")
    groups = send2.shape[1]
    rows = pattern_ref.shape[0]
    count = n * own // LANES
    chunk = groups * count
    pieces = max(groups, 2)
    split = pieces // groups
    piece_rows = chunk // pieces
    half = pieces // 2

    def peer(d):
        return me ^ d

    def fellow(e):
        return lax.rem(group + e, m)

    loads = [
        pltpu.make_async_copy(source, target, load_sem.at[k])
        for k, (source, target) in enumerate(
            ((wave_hbm, wave_ref), (pattern_hbm, pattern_ref), (lags_hbm, lags_ref), (present_hbm, present_ref))
        )
    ]
    for load in loads:
        load.start()

    barrier = pltpu.get_barrier_semaphore()
    for d in range(n - 1, 0, -1):
        pl.semaphore_signal(barrier, inc=1, device_id={"sta": peer(d), "tpl": group}, device_id_type=MESH)
    for e in range(1, m):
        pl.semaphore_signal(barrier, inc=1, device_id={"sta": me, "tpl": fellow(e)}, device_id_type=MESH)

    bands = []
    low = 1
    while low < n:
        bands.append((low, min(2 * low, n)))
        low *= 2
    if len(bands) > 2:
        bands[:2] = [(1, bands[1][1])]

    def copy1(d, band):
        return pltpu.make_async_remote_copy(
            src_ref=packed.at[d],
            dst_ref=recv1.at[d],
            send_sem=send_sem.at[0],
            recv_sem=recv1_sem.at[band],
            device_id={"sta": peer(d), "tpl": group},
            device_id_type=MESH,
        )

    def all1(low, high, band):
        return pltpu.make_async_remote_copy(
            src_ref=packed.at[pl.ds(low, high - low)],
            dst_ref=recv1.at[pl.ds(low, high - low)],
            send_sem=send_sem.at[0],
            recv_sem=recv1_sem.at[band],
            device_id={"sta": peer(1), "tpl": group},
            device_id_type=MESH,
        )

    def copy2(d):
        return pltpu.make_async_remote_copy(
            src_ref=send2.at[peer(d)],
            dst_ref=recv2.at[me],
            send_sem=send_sem.at[1],
            recv_sem=recv2_sem,
            device_id={"sta": peer(d), "tpl": group},
            device_id_type=MESH,
        )

    def all2():
        return pltpu.make_async_remote_copy(
            src_ref=send2.at[pl.ds(1, n - 1)],
            dst_ref=recv2.at[pl.ds(1, n - 1)],
            send_sem=send_sem.at[1],
            recv_sem=recv2_sem,
            device_id={"sta": peer(1), "tpl": group},
            device_id_type=MESH,
        )

    def copy3(e, d):
        return pltpu.make_async_remote_copy(
            src_ref=send3.at[peer(d)],
            dst_ref=recv3.at[e - 1, d],
            send_sem=send_sem.at[2],
            recv_sem=recv3_sem,
            device_id={"sta": peer(d), "tpl": fellow(e)},
            device_id_type=MESH,
        )

    def all3():
        return pltpu.make_async_remote_copy(
            src_ref=recv3,
            dst_ref=recv3,
            send_sem=send_sem.at[2],
            recv_sem=recv3_sem,
            device_id={"sta": peer(1), "tpl": group},
            device_id_type=MESH,
        )

    loads[0].wait()
    loads[1].wait()
    correlate(blocks, stride, wave_ref, pattern_ref, record, hankel, corr)

    loads[2].wait()
    loads[3].wait()
    lane = lax.broadcasted_iota(jnp.int32, (piece_rows, LANES), 1)

    def shifted(d):
        found = []
        for p in range(pieces):
            t = peer(d) * groups + p // split
            lag = lags_ref[t]
            begin = t * stride + (lag >> 7) + (p % split) * piece_rows
            rest = lag & (LANES - 1)
            near = corr[pl.ds(begin, piece_rows), :]
            after = corr[pl.ds(begin + 1, piece_rows), :]
            joined = pltpu.roll(jnp.where(lane >= rest, near, after), (LANES - rest) & (LANES - 1), 1)
            found.append(joined * present_ref[t].astype(jnp.float32))
        return found

    batch = max(n // 4, 1)
    order = list(range(n - 1, 0, -1))
    for begin in range(0, n - 1, batch):
        for d in order[begin : begin + batch]:
            encode(shifted(d), packed, d)
        if begin == 0:
            pl.semaphore_wait(barrier, n + m - 2)
        for d in order[begin : begin + batch]:
            band = next(k for k, (a, b) in enumerate(bands) if a <= d < b)
            copy1(d, band).start()
    total = shifted(0)
    for k, (low, high) in enumerate(bands):
        all1(low, high, k).wait_recv()
        for d in range(low, high):
            total = [a + b for a, b in zip(total, decode(recv1, d, half, piece_rows))]
    stack = jnp.concatenate(total, axis=0)
    scales = deviation_scale(stack, groups, n * own)
    scored[chunk:, :] = jnp.zeros((8, LANES), jnp.float32)
    for t in range(groups):
        scored[t * count : (t + 1) * count, :] = stack[t * count : (t + 1) * count, :] / scales[t]
    scale = jnp.concatenate(scales, axis=0)
    lane = lax.broadcasted_iota(jnp.int32, (groups, LANES), 1)
    for j in range(n):
        begin, rest = divmod(own * j, LANES)
        near = scored[pl.ds(begin, groups, stride=count), :]
        if rest:
            after = scored[pl.ds(begin + 1, groups, stride=count), :]
            near = pltpu.roll(jnp.where(lane >= rest, near, after), LANES - rest, 1)
        send2[j] = jnp.where(lane < own, near, scale)
        send3[j] = jnp.max(near, axis=0, keepdims=True)

    if m == 2:
        for d in range(n - 1, -1, -1):
            copy3(1, d).start()
    else:
        for e in range(1, m):

            def start3(d, carry):
                copy3(e, d).start()
                return carry

            lax.fori_loop(0, n, start3, 0)
    for d in range(n - 1, 0, -1):
        copy2(d).start()
    recv2[me] = send2[me]
    all1(1, n, 0).wait_send()

    all2().wait_recv()
    top = recv2[0]
    out_ref[:groups, :] = top
    for i in range(1, n):
        out_ref[i * groups : (i + 1) * groups, :] = recv2[i]
        top = jnp.maximum(top, recv2[i])
    top = jnp.max(top, axis=0, keepdims=True)
    if m > 1:
        all3().wait_recv()
        for e in range(m - 1):
            top = jnp.maximum(top, jnp.max(recv3[e], axis=0))
    lane = lax.broadcasted_iota(jnp.int32, (8, LANES), 1)
    moved_top = jnp.broadcast_to(pltpu.roll(top, LANES // 2, 1), (8, LANES))
    out_ref[:8, :] = jnp.where(lane < LANES // 2, out_ref[:8, :], moved_top)

    all2().wait_send()
    if m > 1:
        all3().wait_send()


def stack_and_score(wave, pattern, lags, present, n, m):
    chans, samples = wave.shape
    rows = pattern.shape[0]
    total = TOUT_DEV * n
    blocks = -(-(total + LAG) // (2 * LANES))
    span = 2 * LANES * (blocks + 1) + LANES
    padded = ceil_to(max(span + LANES, samples), LANES)
    count = total // LANES
    stride = max(2 * blocks, LAG // LANES + count + 2) | 1
    groups = rows // n
    chunk = groups * count
    words = chunk // 2 + 1
    vmem = pl.BlockSpec(memory_space=pltpu.VMEM)
    return pl.pallas_call(
        functools.partial(stack_kernel, n, m, TOUT_DEV, blocks, stride),
        out_shape=pltpu.VMEM((rows, LANES), jnp.float32),
        in_specs=[pl.BlockSpec(memory_space=pltpu.HBM)] * 4,
        out_specs=vmem,
        scratch_shapes=[
            pltpu.SMEM(lags.shape, lags.dtype),
            pltpu.SMEM(present.shape, present.dtype),
            pltpu.VMEM(wave.shape, wave.dtype),
            pltpu.VMEM(pattern.shape, pattern.dtype),
            pltpu.SemaphoreType.DMA((4,)),
            pltpu.VMEM((chans, padded), jnp.float32),
            pltpu.VMEM((chans, LANES, span), jnp.bfloat16),
            pltpu.VMEM((rows * stride, LANES), jnp.float32),
            pltpu.VMEM((n, words, LANES), jnp.int32),
            pltpu.VMEM((n, words, LANES), jnp.int32),
            pltpu.VMEM((chunk + 8, LANES), jnp.float32),
            pltpu.VMEM((n, groups, LANES), jnp.float32),
            pltpu.VMEM((n, groups, LANES), jnp.float32),
            pltpu.VMEM((n, 1, LANES), jnp.float32),
            pltpu.VMEM((max(m - 1, 1), n, 1, LANES), jnp.float32),
            pltpu.SemaphoreType.DMA((3,)),
            pltpu.SemaphoreType.DMA((max((n - 1).bit_length() - 1, 1),)),
            pltpu.SemaphoreType.DMA,
            pltpu.SemaphoreType.DMA,
        ],
        compiler_params=pltpu.CompilerParams(collective_id=0, has_side_effects=True),
    )(lags, present, wave, pattern)


def finish_kernel(grid_ref, score_ref, scale_ref, peak_ref):
    own, rows = score_ref.shape
    turned = grid_ref[...].T
    score_ref[...] = turned[:own, :]
    scale_ref[...] = turned[own, :]
    peak_ref[...] = grid_ref[0, LANES // 2 : LANES // 2 + own]


def on_device(waveform, templates, lags, present):
    n, m = lax.axis_size("sta"), lax.axis_size("tpl")
    rows = templates.shape[0]
    grid = stack_and_score(waveform[0], templates[:, 0, :], lags[:, 0], present[:, 0], n, m)
    return pl.pallas_call(
        finish_kernel,
        out_shape=(
            jax.ShapeDtypeStruct((TOUT_DEV, rows), jnp.float32),
            jax.ShapeDtypeStruct((rows,), jnp.float32),
            jax.ShapeDtypeStruct((TOUT_DEV,), jnp.float32),
        ),
        in_specs=[pl.BlockSpec(memory_space=pltpu.VMEM)],
        compiler_params=pltpu.CompilerParams(vmem_limit_bytes=VMEM_LIMIT),
    )(grid)


def solution(mesh):
    placed = (P("sta", None, None), P("tpl", "sta", None), P("tpl", "sta"), P("tpl", "sta"))
    return jax.shard_map(
        on_device,
        mesh=mesh,
        in_specs=placed,
        out_specs=(P("sta", "tpl"), P("tpl"), P("sta")),
        check_vma=False,
    )
```

```python
import functools

import jax
import jax.numpy as jnp
from jax import lax
from jax.experimental import pallas as pl
from jax.experimental.pallas import tpu as pltpu
from jax.sharding import PartitionSpec as P

LEN = 512
LAG = 3000
BINS = 1024
TOUT_DEV = 48
LANES = 128
VMEM_LIMIT = 16 * 1024 * 1024
MESH = pl.DeviceIdType.MESH


def ceil_to(value, step):
    return -(-value // step) * step


def build_hankel(record, hankel, first, last):
    row = lax.broadcasted_iota(jnp.int32, (16, LANES), 0)
    back = (lax.broadcasted_iota(jnp.int32, (16, LANES), 1) + row - 2 * (row & 7)).astype(jnp.float32).astype(jnp.bfloat16)
    back = jnp.concatenate([back] * (last - first), axis=1)

    def turned(c, j, a):
        line = jnp.broadcast_to(record[c : c + 1, j * LANES : (j + 1) * LANES], (8, LANES))
        return pltpu.roll(line, LANES - 7 - 8 * a, 1, stride=1, stride_axis=0)

    for c in range(hankel.shape[0]):
        for g in range(LANES // 16):
            halves = [jnp.concatenate([turned(c, j, a) for j in range(first, last + 1)], axis=1) for a in (2 * g, 2 * g + 1)]
            both = jnp.concatenate(halves, axis=0).astype(jnp.bfloat16)
            hankel[c, 16 * g : 16 * g + 16, first * LANES : last * LANES] = jnp.where(
                back < float(LANES - 7 - 16 * g), both[:, :-LANES], both[:, LANES:]
            )


def reverse_eights(pattern):
    rows, width = pattern.shape
    source = lax.broadcasted_iota(jnp.int32, (LANES, LANES), 0)
    target = lax.broadcasted_iota(jnp.int32, (LANES, LANES), 1)
    swap = (source == (target ^ 7)).astype(jnp.float32).astype(jnp.bfloat16)
    chunks = jnp.concatenate([pattern[:, k * LANES : (k + 1) * LANES] for k in range(width // LANES)], axis=0)
    turned = jnp.dot(chunks, swap, preferred_element_type=jnp.float32).astype(jnp.bfloat16)
    return [turned[k * rows : (k + 1) * rows] for k in range(width // LANES)]


def correlate(blocks, stride, wave_ref, pattern_ref, record, hankel, corr):
    chans, samples = wave_ref.shape
    rows = pattern_ref.shape[0]
    span = hankel.shape[2]
    record[...] = jnp.zeros_like(record)
    record[:, :samples] = wave_ref[...].astype(jnp.float32)
    pattern = pattern_ref[...]
    wide = pattern.astype(jnp.float32)
    factor = 1.0 / jnp.sqrt(jnp.sum(wide * wide, axis=1, keepdims=True) + 1e-06)
    depth = 2 * LANES
    chunks = reverse_eights(pattern)
    per = LEN // LANES
    stacked = []
    for c in range(chans):
        halves = [jnp.concatenate([chunks[c * per + 2 * h + q] for q in range(2)], axis=1) for h in range(LEN // depth)]
        stacked.append(jnp.concatenate(halves, axis=0))
    built = 0
    pending = None
    starts = list(range(0, blocks + 1, 16))
    pending = None

    def upto(k):
        last = min(starts[k] + 16, blocks + 1) if k < len(starts) else blocks + 1
        return depth * last + LANES

    for k, first in enumerate(starts):
        width = depth * (min(first + 16, blocks + 1) - first)
        need = upto(k + 0)
        if need > built:
            build_hankel(record, hankel, built // LANES, need // LANES)
        built = need
        for b in range(first, first + width // depth):
            piece = None
            for c in range(chans):
                start = depth * b
                columns = jnp.concatenate([hankel[c, :, start + LANES * q : start + LANES * q + depth] for q in range(2)], axis=0)
                part = jnp.dot(stacked[c], columns, preferred_element_type=jnp.float32)
                piece = part if piece is None else piece + part
            if b:
                total = pending + piece[rows:] * factor
                corr[pl.ds(2 * b - 2, rows, stride=stride), :] = total[:, :LANES]
                corr[pl.ds(2 * b - 1, rows, stride=stride), :] = total[:, LANES:]
            pending = piece[:rows] * factor


FINE = 16


def deviation_scale(stack, groups, total):
    width = 512.0 / BINS
    count = stack.shape[0] // groups
    position = jnp.clip(jnp.abs(stack) / width - 0.5, 0.0, BINS - 1.0)
    lower = jnp.minimum(jnp.floor(position), BINS - 2.0)
    share = position - lower
    head = share.astype(jnp.bfloat16).astype(jnp.float32)
    tail = share - head
    coarse = jnp.floor(lower * (1.0 / FINE))
    fine = lower - FINE * coarse
    broad = lax.broadcasted_iota(jnp.int32, (BINS // FINE, LANES), 0).astype(jnp.float32)
    few = lax.broadcasted_iota(jnp.int32, (FINE, LANES), 0).astype(jnp.float32)
    row = lax.broadcasted_iota(jnp.int32, (FINE, LANES), 0)
    lane = lax.broadcasted_iota(jnp.int32, (FINE, LANES), 1)
    scales = []
    for t in range(groups):
        below, weights = [], []
        for r in range(t * count, (t + 1) * count):
            below.append((coarse[r : r + 1, :] <= broad).astype(jnp.float32).astype(jnp.bfloat16))
            upto = (fine[r : r + 1, :] <= few).astype(jnp.float32)
            same = fine[r : r + 1, :] == few
            parts = [upto, same.astype(jnp.float32), jnp.where(same, head[r : r + 1, :], 0.0), jnp.where(same, tail[r : r + 1, :], 0.0)]
            weights.append(jnp.concatenate(parts, axis=0).astype(jnp.bfloat16))
        weight = jnp.concatenate(weights, axis=1)
        below = jnp.concatenate(below, axis=1)
        found = lax.dot_general(weight, below, (((1,), (1,)), ((), ())), preferred_element_type=jnp.float32)
        if found.shape[1] < LANES:
            found = jnp.concatenate([found, jnp.zeros((found.shape[0], LANES - found.shape[1]), jnp.float32)], axis=1)
        upto, same = found[:FINE], found[FINE : 2 * FINE]
        part = found[2 * FINE : 3 * FINE] + found[3 * FINE :]
        upto_left = jnp.where(lane >= 1, pltpu.roll(upto, 1, 1), 0.0)
        same_left = jnp.where(lane >= 1, pltpu.roll(same, 1, 1), 0.0)
        part_left = jnp.where(lane >= 1, pltpu.roll(part, 1, 1), 0.0)
        part_far = jnp.where(lane >= 2, pltpu.roll(part, 2, 1), 0.0)
        held = same - same_left
        moved = part - part_left
        spilled = pltpu.roll(jnp.where(row == FINE - 1, part_left - part_far, moved), 1, 0)
        counts = held - moved + spilled
        prior = upto_left[FINE - 1 : FINE, :]
        earlier = prior + (upto - upto_left) - held - spilled
        portion = jnp.clip((0.5 * total - earlier) / jnp.maximum(counts, 1.0), 0.0, 1.0)
        portion = jnp.where(lane < BINS // FINE, portion, 0.0)
        portion = jnp.sum(portion, axis=0, keepdims=True)
        scales.append(1.4826 * (width * jnp.sum(portion, axis=1, keepdims=True)))
    return scales


LEVELS = 32600.0
ROUNDER = 12582912.0
CODE_STEP = 64.0


def encode(pieces, target, slot):
    half = len(pieces) // 2
    rows = pieces[0].shape[0]
    most = jnp.abs(pieces[0])
    for piece in pieces[1:]:
        most = jnp.maximum(most, jnp.abs(piece))
    most = jnp.maximum(jnp.max(most, axis=0, keepdims=True), 1e-30)
    code = jnp.floor(jnp.log2(most) * CODE_STEP) + 1.0
    inverse = LEVELS * jnp.exp2(code * (-1.0 / CODE_STEP))
    for p in range(half):
        high = (pieces[p] * inverse + ROUNDER).astype(jnp.int32)
        low = (pieces[p + half] * inverse + ROUNDER).astype(jnp.int32)
        target[slot, p * rows : (p + 1) * rows, :] = (high << 16) | (low & 65535)
    target[slot, half * rows : half * rows + 1, :] = code.astype(jnp.int32)


def decode(source, slot, half, rows):
    code = source[slot, half * rows : half * rows + 1, :].astype(jnp.float32)
    scale = jnp.exp2(code * (1.0 / CODE_STEP)) * (1.0 / LEVELS)
    highs, lows = [], []
    for p in range(half):
        word = source[slot, p * rows : (p + 1) * rows, :]
        highs.append((word >> 16).astype(jnp.float32) * scale)
        lows.append(((word << 16) >> 16).astype(jnp.float32) * scale)
    return highs + lows


def stack_kernel(n, m, own, blocks, stride, lags_hbm, present_hbm, wave_hbm, pattern_hbm, out_ref, lags_ref, present_ref, wave_ref, pattern_ref, load_sem, record, hankel, corr, packed, recv1, scored, send2, recv2, send3, recv3, send_sem, recv1_sem, recv2_sem, recv3_sem):
    me, group = lax.axis_index("sta"), lax.axis_index("tpl")
    groups = send2.shape[1]
    rows = pattern_ref.shape[0]
    count = n * own // LANES
    chunk = groups * count
    pieces = max(groups, 2)
    split = pieces // groups
    piece_rows = chunk // pieces
    half = pieces // 2

    def peer(d):
        return me ^ d

    def fellow(e):
        return lax.rem(group + e, m)

    loads = [
        pltpu.make_async_copy(source, target, load_sem.at[k])
        for k, (source, target) in enumerate(
            ((wave_hbm, wave_ref), (pattern_hbm, pattern_ref), (lags_hbm, lags_ref), (present_hbm, present_ref))
        )
    ]
    for load in loads:
        load.start()

    barrier = pltpu.get_barrier_semaphore()
    for d in range(n - 1, 0, -1):
        pl.semaphore_signal(barrier, inc=1, device_id={"sta": peer(d), "tpl": group}, device_id_type=MESH)
    for e in range(1, m):
        pl.semaphore_signal(barrier, inc=1, device_id={"sta": me, "tpl": fellow(e)}, device_id_type=MESH)

    bands = []
    low = 1
    while low < n:
        bands.append((low, min(2 * low, n)))
        low *= 2
    if len(bands) > 2:
        bands[:2] = [(1, bands[1][1])]

    def copy1(d, band):
        return pltpu.make_async_remote_copy(
            src_ref=packed.at[d],
            dst_ref=recv1.at[d],
            send_sem=send_sem.at[0],
            recv_sem=recv1_sem.at[band],
            device_id={"sta": peer(d), "tpl": group},
            device_id_type=MESH,
        )

    def all1(low, high, band):
        return pltpu.make_async_remote_copy(
            src_ref=packed.at[pl.ds(low, high - low)],
            dst_ref=recv1.at[pl.ds(low, high - low)],
            send_sem=send_sem.at[0],
            recv_sem=recv1_sem.at[band],
            device_id={"sta": peer(1), "tpl": group},
            device_id_type=MESH,
        )

    def copy2(d):
        return pltpu.make_async_remote_copy(
            src_ref=send2.at[peer(d)],
            dst_ref=recv2.at[me],
            send_sem=send_sem.at[1],
            recv_sem=recv2_sem,
            device_id={"sta": peer(d), "tpl": group},
            device_id_type=MESH,
        )

    def all2():
        return pltpu.make_async_remote_copy(
            src_ref=send2.at[pl.ds(1, n - 1)],
            dst_ref=recv2.at[pl.ds(1, n - 1)],
            send_sem=send_sem.at[1],
            recv_sem=recv2_sem,
            device_id={"sta": peer(1), "tpl": group},
            device_id_type=MESH,
        )

    def copy3(e, d):
        return pltpu.make_async_remote_copy(
            src_ref=send3.at[peer(d)],
            dst_ref=recv3.at[e - 1, d],
            send_sem=send_sem.at[2],
            recv_sem=recv3_sem,
            device_id={"sta": peer(d), "tpl": fellow(e)},
            device_id_type=MESH,
        )

    def all3():
        return pltpu.make_async_remote_copy(
            src_ref=recv3,
            dst_ref=recv3,
            send_sem=send_sem.at[2],
            recv_sem=recv3_sem,
            device_id={"sta": peer(1), "tpl": group},
            device_id_type=MESH,
        )

    loads[0].wait()
    loads[1].wait()
    correlate(blocks, stride, wave_ref, pattern_ref, record, hankel, corr)

    loads[2].wait()
    loads[3].wait()
    lane = lax.broadcasted_iota(jnp.int32, (piece_rows, LANES), 1)

    def shifted(d):
        found = []
        for p in range(pieces):
            t = peer(d) * groups + p // split
            lag = lags_ref[t]
            begin = t * stride + (lag >> 7) + (p % split) * piece_rows
            rest = lag & (LANES - 1)
            near = corr[pl.ds(begin, piece_rows), :]
            after = corr[pl.ds(begin + 1, piece_rows), :]
            joined = pltpu.roll(jnp.where(lane >= rest, near, after), (LANES - rest) & (LANES - 1), 1)
            found.append(joined * present_ref[t].astype(jnp.float32))
        return found

    batch = max(n // 4, 1)
    order = list(range(n - 1, 0, -1))
    for begin in range(0, n - 1, batch):
        for d in order[begin : begin + batch]:
            encode(shifted(d), packed, d)
        if begin == 0:
            pl.semaphore_wait(barrier, n + m - 2)
        for d in order[begin : begin + batch]:
            band = next(k for k, (a, b) in enumerate(bands) if a <= d < b)
            copy1(d, band).start()
    total = shifted(0)
    for k, (low, high) in enumerate(bands):
        all1(low, high, k).wait_recv()
        for d in range(low, high):
            total = [a + b for a, b in zip(total, decode(recv1, d, half, piece_rows))]
    for p in range(pieces):
        scored[p * piece_rows : (p + 1) * piece_rows, :] = total[p]
    scored[chunk:, :] = jnp.zeros((8, LANES), jnp.float32)
    stack = scored[:chunk, :]
    lane = lax.broadcasted_iota(jnp.int32, (groups, LANES), 1)
    views = []
    for j in range(n):
        begin, rest = divmod(own * j, LANES)
        near = scored[pl.ds(begin, groups, stride=count), :]
        if rest:
            after = scored[pl.ds(begin + 1, groups, stride=count), :]
            near = pltpu.roll(jnp.where(lane >= rest, near, after), LANES - rest, 1)
        views.append(near)
    scale = jnp.concatenate(deviation_scale(stack, groups, n * own), axis=0)
    inverse = 1.0 / scale
    for j in range(n):
        near = views[j] * inverse
        send2[j] = jnp.where(lane < own, near, scale)
        send3[j] = jnp.max(near, axis=0, keepdims=True)

    if m == 2:
        for d in range(n - 1, -1, -1):
            copy3(1, d).start()
    else:
        for e in range(1, m):

            def start3(d, carry):
                copy3(e, d).start()
                return carry

            lax.fori_loop(0, n, start3, 0)
    for d in range(n - 1, 0, -1):
        copy2(d).start()
    recv2[me] = send2[me]
    all1(1, n, 0).wait_send()

    all2().wait_recv()
    top = recv2[0]
    out_ref[:groups, :] = top
    for i in range(1, n):
        out_ref[i * groups : (i + 1) * groups, :] = recv2[i]
        top = jnp.maximum(top, recv2[i])
    top = jnp.max(top, axis=0, keepdims=True)
    if m > 1:
        all3().wait_recv()
        for e in range(m - 1):
            top = jnp.maximum(top, jnp.max(recv3[e], axis=0))
    lane = lax.broadcasted_iota(jnp.int32, (8, LANES), 1)
    moved_top = jnp.broadcast_to(pltpu.roll(top, LANES // 2, 1), (8, LANES))
    out_ref[:8, :] = jnp.where(lane < LANES // 2, out_ref[:8, :], moved_top)

    all2().wait_send()
    if m > 1:
        all3().wait_send()


def stack_and_score(wave, pattern, lags, present, n, m):
    chans, samples = wave.shape
    rows = pattern.shape[0]
    total = TOUT_DEV * n
    blocks = -(-(total + LAG) // (2 * LANES))
    span = 2 * LANES * (blocks + 1) + LANES
    padded = ceil_to(max(span + LANES, samples), LANES)
    count = total // LANES
    stride = max(2 * blocks, LAG // LANES + count + 2) | 1
    groups = rows // n
    chunk = groups * count
    words = chunk // 2 + 1
    vmem = pl.BlockSpec(memory_space=pltpu.VMEM)
    return pl.pallas_call(
        functools.partial(stack_kernel, n, m, TOUT_DEV, blocks, stride),
        out_shape=pltpu.VMEM((rows, LANES), jnp.float32),
        in_specs=[pl.BlockSpec(memory_space=pltpu.HBM)] * 4,
        out_specs=vmem,
        scratch_shapes=[
            pltpu.SMEM(lags.shape, lags.dtype),
            pltpu.SMEM(present.shape, present.dtype),
            pltpu.VMEM(wave.shape, wave.dtype),
            pltpu.VMEM(pattern.shape, pattern.dtype),
            pltpu.SemaphoreType.DMA((4,)),
            pltpu.VMEM((chans, padded), jnp.float32),
            pltpu.VMEM((chans, LANES, span), jnp.bfloat16),
            pltpu.VMEM((rows * stride, LANES), jnp.float32),
            pltpu.VMEM((n, words, LANES), jnp.int32),
            pltpu.VMEM((n, words, LANES), jnp.int32),
            pltpu.VMEM((chunk + 8, LANES), jnp.float32),
            pltpu.VMEM((n, groups, LANES), jnp.float32),
            pltpu.VMEM((n, groups, LANES), jnp.float32),
            pltpu.VMEM((n, 1, LANES), jnp.float32),
            pltpu.VMEM((max(m - 1, 1), n, 1, LANES), jnp.float32),
            pltpu.SemaphoreType.DMA((3,)),
            pltpu.SemaphoreType.DMA((max((n - 1).bit_length() - 1, 1),)),
            pltpu.SemaphoreType.DMA,
            pltpu.SemaphoreType.DMA,
        ],
        compiler_params=pltpu.CompilerParams(collective_id=0, has_side_effects=True),
    )(lags, present, wave, pattern)


def finish_kernel(grid_ref, score_ref, scale_ref, peak_ref):
    own, rows = score_ref.shape
    turned = grid_ref[...].T
    score_ref[...] = turned[:own, :]
    scale_ref[...] = turned[own, :]
    peak_ref[...] = grid_ref[0, LANES // 2 : LANES // 2 + own]


def on_device(waveform, templates, lags, present):
    n, m = lax.axis_size("sta"), lax.axis_size("tpl")
    rows = templates.shape[0]
    grid = stack_and_score(waveform[0], templates[:, 0, :], lags[:, 0], present[:, 0], n, m)
    return pl.pallas_call(
        finish_kernel,
        out_shape=(
            jax.ShapeDtypeStruct((TOUT_DEV, rows), jnp.float32),
            jax.ShapeDtypeStruct((rows,), jnp.float32),
            jax.ShapeDtypeStruct((TOUT_DEV,), jnp.float32),
        ),
        in_specs=[pl.BlockSpec(memory_space=pltpu.VMEM)],
        compiler_params=pltpu.CompilerParams(vmem_limit_bytes=VMEM_LIMIT),
    )(grid)


def solution(mesh):
    placed = (P("sta", None, None), P("tpl", "sta", None), P("tpl", "sta"), P("tpl", "sta"))
    return jax.shard_map(
        on_device,
        mesh=mesh,
        in_specs=placed,
        out_specs=(P("sta", "tpl"), P("tpl"), P("sta")),
        check_vma=False,
    )
```

```python
import functools

import jax
import jax.numpy as jnp
from jax import lax
from jax.experimental import pallas as pl
from jax.experimental.pallas import tpu as pltpu
from jax.sharding import PartitionSpec as P

LEN = 512
LAG = 3000
BINS = 1024
TOUT_DEV = 48
LANES = 128
VMEM_LIMIT = 16 * 1024 * 1024
MESH = pl.DeviceIdType.MESH


def ceil_to(value, step):
    return -(-value // step) * step


def build_hankel(record, hankel, first, last):
    row = lax.broadcasted_iota(jnp.int32, (16, LANES), 0)
    back = (lax.broadcasted_iota(jnp.int32, (16, LANES), 1) + row - 2 * (row & 7)).astype(jnp.float32).astype(jnp.bfloat16)
    back = jnp.concatenate([back] * (last - first), axis=1)

    def turned(c, j, a):
        line = jnp.broadcast_to(record[c : c + 1, j * LANES : (j + 1) * LANES], (8, LANES))
        return pltpu.roll(line, LANES - 7 - 8 * a, 1, stride=1, stride_axis=0)

    for c in range(hankel.shape[0]):
        for g in range(LANES // 16):
            halves = [jnp.concatenate([turned(c, j, a) for j in range(first, last + 1)], axis=1) for a in (2 * g, 2 * g + 1)]
            both = jnp.concatenate(halves, axis=0).astype(jnp.bfloat16)
            hankel[c, 16 * g : 16 * g + 16, first * LANES : last * LANES] = jnp.where(
                back < float(LANES - 7 - 16 * g), both[:, :-LANES], both[:, LANES:]
            )


def reverse_eights(pattern):
    rows, width = pattern.shape
    source = lax.broadcasted_iota(jnp.int32, (LANES, LANES), 0)
    target = lax.broadcasted_iota(jnp.int32, (LANES, LANES), 1)
    swap = (source == (target ^ 7)).astype(jnp.float32).astype(jnp.bfloat16)
    chunks = jnp.concatenate([pattern[:, k * LANES : (k + 1) * LANES] for k in range(width // LANES)], axis=0)
    turned = jnp.dot(chunks, swap, preferred_element_type=jnp.float32).astype(jnp.bfloat16)
    return [turned[k * rows : (k + 1) * rows] for k in range(width // LANES)]


def correlate(blocks, stride, wave_ref, pattern_ref, record, hankel, corr, load):
    chans, samples = wave_ref.shape
    rows = pattern_ref.shape[0]
    span = hankel.shape[2]
    record[...] = jnp.zeros_like(record)
    record[:, :samples] = wave_ref[...].astype(jnp.float32)
    depth = 2 * LANES
    built = depth * min(4, blocks + 1) + LANES
    build_hankel(record, hankel, 0, built // LANES)
    load.wait()
    pattern = pattern_ref[...]
    wide = pattern.astype(jnp.float32)
    factor = 1.0 / jnp.sqrt(jnp.sum(wide * wide, axis=1, keepdims=True) + 1e-06)
    chunks = reverse_eights(pattern)
    per = LEN // LANES
    stacked = []
    for c in range(chans):
        halves = [jnp.concatenate([chunks[c * per + 2 * h + q] for q in range(2)], axis=1) for h in range(LEN // depth)]
        stacked.append(jnp.concatenate(halves, axis=0))
    starts = list(range(0, blocks + 1, 2))
    pending = None

    def upto(k):
        last = min(starts[k] + 2, blocks + 1) if k < len(starts) else blocks + 1
        return depth * last + LANES

    for k, first in enumerate(starts):
        width = depth * (min(first + 2, blocks + 1) - first)
        need = upto(k + 1)
        if need > built:
            build_hankel(record, hankel, built // LANES, need // LANES)
        built = need
        for b in range(first, first + width // depth):
            piece = None
            for c in range(chans):
                start = depth * b
                columns = jnp.concatenate([hankel[c, :, start + LANES * q : start + LANES * q + depth] for q in range(2)], axis=0)
                part = jnp.dot(stacked[c], columns, preferred_element_type=jnp.float32)
                piece = part if piece is None else piece + part
            if b:
                total = pending + piece[rows:] * factor
                corr[pl.ds(2 * b - 2, rows, stride=stride), :] = total[:, :LANES]
                corr[pl.ds(2 * b - 1, rows, stride=stride), :] = total[:, LANES:]
            pending = piece[:rows] * factor


FINE = 16


def deviation_scale(stack, groups, total):
    width = 512.0 / BINS
    count = stack.shape[0] // groups
    position = jnp.clip(jnp.abs(stack) / width - 0.5, 0.0, BINS - 1.0)
    lower = jnp.minimum(jnp.floor(position), BINS - 2.0)
    share = position - lower
    head = share.astype(jnp.bfloat16).astype(jnp.float32)
    tail = share - head
    coarse = jnp.floor(lower * (1.0 / FINE))
    fine = lower - FINE * coarse
    broad = lax.broadcasted_iota(jnp.int32, (BINS // FINE, LANES), 0).astype(jnp.float32)
    few = lax.broadcasted_iota(jnp.int32, (FINE, LANES), 0).astype(jnp.float32)
    row = lax.broadcasted_iota(jnp.int32, (FINE, LANES), 0)
    lane = lax.broadcasted_iota(jnp.int32, (FINE, LANES), 1)
    scales = []
    for t in range(groups):
        below, weights = [], []
        for r in range(t * count, (t + 1) * count):
            below.append((coarse[r : r + 1, :] <= broad).astype(jnp.float32).astype(jnp.bfloat16))
            upto = (fine[r : r + 1, :] <= few).astype(jnp.float32)
            same = fine[r : r + 1, :] == few
            parts = [upto, same.astype(jnp.float32), jnp.where(same, head[r : r + 1, :], 0.0), jnp.where(same, tail[r : r + 1, :], 0.0)]
            weights.append(jnp.concatenate(parts, axis=0).astype(jnp.bfloat16))
        weight = jnp.concatenate(weights, axis=1)
        below = jnp.concatenate(below, axis=1)
        found = lax.dot_general(weight, below, (((1,), (1,)), ((), ())), preferred_element_type=jnp.float32)
        if found.shape[1] < LANES:
            found = jnp.concatenate([found, jnp.zeros((found.shape[0], LANES - found.shape[1]), jnp.float32)], axis=1)
        upto, same = found[:FINE], found[FINE : 2 * FINE]
        part = found[2 * FINE : 3 * FINE] + found[3 * FINE :]
        upto_left = jnp.where(lane >= 1, pltpu.roll(upto, 1, 1), 0.0)
        same_left = jnp.where(lane >= 1, pltpu.roll(same, 1, 1), 0.0)
        part_left = jnp.where(lane >= 1, pltpu.roll(part, 1, 1), 0.0)
        part_far = jnp.where(lane >= 2, pltpu.roll(part, 2, 1), 0.0)
        held = same - same_left
        moved = part - part_left
        spilled = pltpu.roll(jnp.where(row == FINE - 1, part_left - part_far, moved), 1, 0)
        counts = held - moved + spilled
        prior = upto_left[FINE - 1 : FINE, :]
        earlier = prior + (upto - upto_left) - held - spilled
        portion = jnp.clip((0.5 * total - earlier) / jnp.maximum(counts, 1.0), 0.0, 1.0)
        portion = jnp.where(lane < BINS // FINE, portion, 0.0)
        portion = jnp.sum(portion, axis=0, keepdims=True)
        scales.append(1.4826 * (width * jnp.sum(portion, axis=1, keepdims=True)))
    return scales


LEVELS = 32600.0
ROUNDER = 12582912.0
CODE_STEP = 64.0


def encode(pieces, target, slot):
    half = len(pieces) // 2
    rows = pieces[0].shape[0]
    codes, inverses = [], []
    for group in (pieces[:half], pieces[half:]):
        most = jnp.abs(group[0])
        for piece in group[1:]:
            most = jnp.maximum(most, jnp.abs(piece))
        most = jnp.maximum(jnp.max(most, axis=0, keepdims=True), 1e-30)
        code = jnp.floor(jnp.log2(most) * CODE_STEP) + 1.0
        inverses.append(LEVELS * jnp.exp2(code * (-1.0 / CODE_STEP)))
        codes.append(code.astype(jnp.int32))
    for p in range(half):
        high = (pieces[p] * inverses[0] + ROUNDER).astype(jnp.int32)
        low = (pieces[p + half] * inverses[1] + ROUNDER).astype(jnp.int32)
        target[slot, p * rows : (p + 1) * rows, :] = (high << 16) | (low & 65535)
    target[slot, half * rows : half * rows + 1, :] = (codes[0] << 16) | (codes[1] & 65535)


def decode(source, slot, half, rows):
    def split(word):
        return (word >> 16).astype(jnp.float32), ((word << 16) >> 16).astype(jnp.float32)

    scales = [jnp.exp2(code * (1.0 / CODE_STEP)) * (1.0 / LEVELS) for code in split(source[slot, half * rows : half * rows + 1, :])]
    highs, lows = [], []
    for p in range(half):
        high, low = split(source[slot, p * rows : (p + 1) * rows, :])
        highs.append(high * scales[0])
        lows.append(low * scales[1])
    return highs + lows


def stack_kernel(n, m, own, blocks, stride, lags_hbm, present_hbm, wave_hbm, pattern_hbm, out_ref, lags_ref, present_ref, wave_ref, pattern_ref, load_sem, record, hankel, corr, packed, recv1, scored, send2, recv2, send3, recv3, send_sem, recv1_sem, recv2_sem, recv3_sem):
    me, group = lax.axis_index("sta"), lax.axis_index("tpl")
    owners = n // 2
    quarter = n // 4
    half = send2.shape[1]
    groups = 2 * half
    rows = pattern_ref.shape[0]
    count = n * own // LANES
    chunk = groups * count
    upper = (me >= owners).astype(jnp.int32)
    virtual = upper * quarter + lax.rem(me, quarter)
    owner = jnp.logical_and(me >= quarter, me < 3 * quarter)
    outer = 1 - owner.astype(jnp.int32)

    def peer(d):
        return me ^ d

    def fellow(e):
        return lax.rem(group + e, m)

    loads = [
        pltpu.make_async_copy(source, target, load_sem.at[k])
        for k, (source, target) in enumerate(
            ((wave_hbm, wave_ref), (pattern_hbm, pattern_ref), (lags_hbm, lags_ref), (present_hbm, present_ref))
        )
    ]
    for load in loads:
        load.start()

    barrier = pltpu.get_barrier_semaphore()

    @pl.when(owner)
    def greet():
        for d in range(n - 1, 0, -1):
            pl.semaphore_signal(barrier, inc=1, device_id={"sta": peer(d), "tpl": group}, device_id_type=MESH)

    for e in range(1, m):
        pl.semaphore_signal(barrier, inc=1, device_id={"sta": me, "tpl": fellow(e)}, device_id_type=MESH)

    def move(source, target, send, recv, sta, tpl):
        return pltpu.make_async_remote_copy(
            src_ref=source,
            dst_ref=target,
            send_sem=send_sem.at[send],
            recv_sem=recv,
            device_id={"sta": sta, "tpl": tpl},
            device_id_type=MESH,
        )

    def copy1(k):
        band = 2 * outer + (1 if k >= quarter else 0)
        return move(packed.at[k], recv1.at[outer * owners + k], 0, recv1_sem.at[band], quarter + (virtual ^ k), group)

    def span1(low, high, band):
        part = recv1.at[pl.ds(low, high - low)]
        return move(part, part, 0, recv1_sem.at[band], peer(1), group)

    def copy2(p):
        return move(send2.at[p], recv2.at[virtual], 1, recv2_sem, p, group)

    def span2(size):
        part = recv2.at[pl.ds(0, size)]
        return move(part, part, 1, recv2_sem, peer(1), group)

    def copy3(e, p):
        return move(send3.at[p], recv3.at[e - 1, virtual], 2, recv3_sem, p, fellow(e))

    loads[0].wait()
    correlate(blocks, stride, wave_ref, pattern_ref, record, hankel, corr, loads[1])

    loads[2].wait()
    loads[3].wait()
    lane = lax.broadcasted_iota(jnp.int32, (count, LANES), 1)

    def shifted(k):
        found = []
        for p in range(groups):
            t = (p // half) * (rows // 2) + (virtual ^ k) * half + p % half
            lag = lags_ref[t]
            begin = t * stride + (lag >> 7)
            rest = lag & (LANES - 1)
            near = corr[pl.ds(begin, count), :]
            after = corr[pl.ds(begin + 1, count), :]
            joined = pltpu.roll(jnp.where(lane >= rest, near, after), (LANES - rest) & (LANES - 1), 1)
            found.append(joined * present_ref[t].astype(jnp.float32))
        return found

    order = sorted(range(1, owners), key=lambda k: (-(k & (quarter // 2)), -k))
    encode(shifted(order[0]), packed, order[0])
    pl.semaphore_wait(barrier, owners + m - 2 + outer)
    copy1(order[0]).start()
    begin, size = 1, 3
    while begin < len(order):
        batch = order[begin : begin + size]
        for k in batch:
            encode(shifted(k), packed, k)
        for k in batch:
            copy1(k).start()
        begin += size

    @pl.when(jnp.logical_not(owner))
    def last():
        encode(shifted(0), packed, 0)
        copy1(0).start()

    @pl.when(owner)
    def serve():
        total = shifted(0)
        for band, low, high in ((0, 1, quarter), (1, quarter, owners), (2, owners, owners + quarter), (3, owners + quarter, n)):
            span1(low, high, band).wait_recv()
            for slot in range(low, high):
                total = [a + b for a, b in zip(total, decode(recv1, slot, half, count))]
        for p in range(groups):
            scored[p * count : (p + 1) * count, :] = total[p]
        scored[chunk:, :] = jnp.zeros((8, LANES), jnp.float32)
        stack = scored[:chunk, :]
        lane = lax.broadcasted_iota(jnp.int32, (half, LANES), 1)
        middle = LANES // 2
        views = []
        for j in range(n):
            begin, rest = divmod(own * j, LANES)
            sides = []
            for side in range(2):
                first = side * half * count + begin
                near = scored[pl.ds(first, half, stride=count), :]
                if rest:
                    after = scored[pl.ds(first + 1, half, stride=count), :]
                    near = jnp.where(lane >= rest, near, after)
                turn = (side * middle - rest) % LANES
                sides.append(pltpu.roll(near, turn, 1) if turn else near)
            views.append(jnp.where(lane < middle, sides[0], sides[1]))
        scales = deviation_scale(stack, groups, n * own)
        scale = jnp.where(lane < middle, jnp.concatenate(scales[:half], axis=0), jnp.concatenate(scales[half:], axis=0))
        inverse = 1.0 / scale

        def ready(targets):
            for j in targets:
                near = views[j] * inverse
                send2[j] = jnp.where((lane & (middle - 1)) < own, near, scale)
                send3[j] = jnp.max(near, axis=0, keepdims=True)

        def leave(targets):
            for p in targets:
                if m == 2:
                    copy3(1, p).start()
                if quarter <= p < 3 * quarter:

                    @pl.when(me != p)
                    def start2():
                        copy2(p).start()

                else:
                    copy2(p).start()

        ready(range(quarter))
        leave(range(quarter))
        ready(range(quarter, n))
        leave(range(quarter, n))
        if m > 2:
            for e in range(1, m):

                def start3(p, carry):
                    copy3(e, p).start()
                    return carry

                lax.fori_loop(0, n, start3, 0)
        recv2[virtual] = send2[me]

    @pl.when(owner)
    def arrive_owner():
        span2(owners - 1).wait_recv()

    @pl.when(jnp.logical_not(owner))
    def arrive():
        span2(owners).wait_recv()

    top = recv2[0]
    for i in range(owners):
        piece = recv2[i]
        out_ref[i * half : (i + 1) * half, :] = piece
        top = jnp.maximum(top, piece)
    out_ref[rows // 2 :, :] = pltpu.roll(out_ref[: rows // 2, :], LANES // 2, 1)
    top = jnp.max(top, axis=0, keepdims=True)
    if m > 1:
        move(recv3, recv3, 2, recv3_sem, peer(1), group).wait_recv()
        for e in range(m - 1):
            top = jnp.maximum(top, jnp.max(recv3[e], axis=0))
    top = jnp.broadcast_to(jnp.maximum(top, pltpu.roll(top, LANES // 2, 1)), (8, LANES))
    lane = lax.broadcasted_iota(jnp.int32, (8, LANES), 1)
    out_ref[:8, :] = jnp.where(lane < LANES // 2, out_ref[:8, :], top)

    @pl.when(jnp.logical_not(owner))
    def drain():
        span1(0, owners, 0).wait_send()

    @pl.when(owner)
    def drain_owner():
        span1(1, owners, 0).wait_send()
        move(send2.at[pl.ds(0, n - 1)], send2.at[pl.ds(0, n - 1)], 1, recv2_sem, peer(1), group).wait_send()
        for e in range(1, m):
            move(send3, send3, 2, recv3_sem, peer(1), group).wait_send()


def stack_and_score(wave, pattern, lags, present, n, m):
    chans, samples = wave.shape
    rows = pattern.shape[0]
    total = TOUT_DEV * n
    blocks = -(-(total + LAG) // (2 * LANES))
    span = 2 * LANES * (blocks + 1) + LANES
    padded = ceil_to(max(span + LANES, samples), LANES)
    count = total // LANES
    stride = max(2 * blocks, LAG // LANES + count + 2) | 1
    owners = n // 2
    groups = rows // owners
    chunk = groups * count
    words = chunk // 2 + 1
    vmem = pl.BlockSpec(memory_space=pltpu.VMEM)
    return pl.pallas_call(
        functools.partial(stack_kernel, n, m, TOUT_DEV, blocks, stride),
        out_shape=pltpu.VMEM((rows, LANES), jnp.float32),
        in_specs=[pl.BlockSpec(memory_space=pltpu.HBM)] * 4,
        out_specs=vmem,
        scratch_shapes=[
            pltpu.SMEM(lags.shape, lags.dtype),
            pltpu.SMEM(present.shape, present.dtype),
            pltpu.VMEM(wave.shape, wave.dtype),
            pltpu.VMEM(pattern.shape, pattern.dtype),
            pltpu.SemaphoreType.DMA((4,)),
            pltpu.VMEM((chans, padded), jnp.float32),
            pltpu.VMEM((chans, LANES, span), jnp.bfloat16),
            pltpu.VMEM((rows * stride, LANES), jnp.float32),
            pltpu.VMEM((owners, words, LANES), jnp.int32),
            pltpu.VMEM((n, words, LANES), jnp.int32),
            pltpu.VMEM((chunk + 8, LANES), jnp.float32),
            pltpu.VMEM((n, groups // 2, LANES), jnp.float32),
            pltpu.VMEM((owners, groups // 2, LANES), jnp.float32),
            pltpu.VMEM((n, 1, LANES), jnp.float32),
            pltpu.VMEM((max(m - 1, 1), owners, 1, LANES), jnp.float32),
            pltpu.SemaphoreType.DMA((3,)),
            pltpu.SemaphoreType.DMA((4,)),
            pltpu.SemaphoreType.DMA,
            pltpu.SemaphoreType.DMA,
        ],
        compiler_params=pltpu.CompilerParams(collective_id=0, has_side_effects=True),
    )(lags, present, wave, pattern)


def finish_kernel(grid_ref, score_ref, scale_ref, peak_ref):
    own, rows = score_ref.shape
    turned = grid_ref[...].T
    score_ref[...] = turned[:own, :]
    scale_ref[...] = turned[own, :]
    peak_ref[...] = grid_ref[0, LANES // 2 : LANES // 2 + own]


def on_device(waveform, templates, lags, present):
    n, m = lax.axis_size("sta"), lax.axis_size("tpl")
    rows = templates.shape[0]
    grid = stack_and_score(waveform[0], templates[:, 0, :], lags[:, 0], present[:, 0], n, m)
    return pl.pallas_call(
        finish_kernel,
        out_shape=(
            jax.ShapeDtypeStruct((TOUT_DEV, rows), jnp.float32),
            jax.ShapeDtypeStruct((rows,), jnp.float32),
            jax.ShapeDtypeStruct((TOUT_DEV,), jnp.float32),
        ),
        in_specs=[pl.BlockSpec(memory_space=pltpu.VMEM)],
        compiler_params=pltpu.CompilerParams(vmem_limit_bytes=VMEM_LIMIT),
    )(grid)


def solution(mesh):
    placed = (P("sta", None, None), P("tpl", "sta", None), P("tpl", "sta"), P("tpl", "sta"))
    return jax.shard_map(
        on_device,
        mesh=mesh,
        in_specs=placed,
        out_specs=(P("sta", "tpl"), P("tpl"), P("sta")),
        check_vma=False,
    )
```

```python
import functools

import jax
import jax.numpy as jnp
from jax import lax
from jax.experimental import pallas as pl
from jax.experimental.pallas import tpu as pltpu
from jax.sharding import PartitionSpec as P

LEN = 512
LAG = 3000
BINS = 1024
TOUT_DEV = 48
LANES = 128
VMEM_LIMIT = 16 * 1024 * 1024
MESH = pl.DeviceIdType.MESH


def ceil_to(value, step):
    return -(-value // step) * step


def build_hankel(record, hankel, first, last):
    row = lax.broadcasted_iota(jnp.int32, (16, LANES), 0)
    back = (lax.broadcasted_iota(jnp.int32, (16, LANES), 1) + row - 2 * (row & 7)).astype(jnp.float32).astype(jnp.bfloat16)
    back = jnp.concatenate([back] * (last - first), axis=1)

    def turned(c, j, a):
        line = jnp.broadcast_to(record[c : c + 1, j * LANES : (j + 1) * LANES], (8, LANES))
        return pltpu.roll(line, LANES - 7 - 8 * a, 1, stride=1, stride_axis=0)

    for c in range(hankel.shape[0]):
        for g in range(LANES // 16):
            halves = [jnp.concatenate([turned(c, j, a) for j in range(first, last + 1)], axis=1) for a in (2 * g, 2 * g + 1)]
            both = jnp.concatenate(halves, axis=0).astype(jnp.bfloat16)
            hankel[c, 16 * g : 16 * g + 16, first * LANES : last * LANES] = jnp.where(
                back < float(LANES - 7 - 16 * g), both[:, :-LANES], both[:, LANES:]
            )


def reverse_eights(pattern):
    rows, width = pattern.shape
    source = lax.broadcasted_iota(jnp.int32, (LANES, LANES), 0)
    target = lax.broadcasted_iota(jnp.int32, (LANES, LANES), 1)
    swap = (source == (target ^ 7)).astype(jnp.float32).astype(jnp.bfloat16)
    chunks = jnp.concatenate([pattern[:, k * LANES : (k + 1) * LANES] for k in range(width // LANES)], axis=0)
    turned = jnp.dot(chunks, swap, preferred_element_type=jnp.float32).astype(jnp.bfloat16)
    return [turned[k * rows : (k + 1) * rows] for k in range(width // LANES)]


def correlate(blocks, stride, wave_ref, pattern_ref, record, hankel, corr, load):
    chans, samples = wave_ref.shape
    rows = pattern_ref.shape[0]
    span = hankel.shape[2]
    record[...] = jnp.zeros_like(record)
    record[:, :samples] = wave_ref[...].astype(jnp.float32)
    depth = 2 * LANES
    built = depth * min(4, blocks + 1) + LANES
    build_hankel(record, hankel, 0, built // LANES)
    load.wait()
    pattern = pattern_ref[...]
    wide = pattern.astype(jnp.float32)
    factor = 1.0 / jnp.sqrt(jnp.sum(wide * wide, axis=1, keepdims=True) + 1e-06)
    chunks = reverse_eights(pattern)
    per = LEN // LANES
    stacked = []
    for c in range(chans):
        halves = [jnp.concatenate([chunks[c * per + 2 * h + q] for q in range(2)], axis=1) for h in range(LEN // depth)]
        stacked.append(jnp.concatenate(halves, axis=0))
    starts = list(range(0, blocks + 1, 2))
    pending = None

    def upto(k):
        last = min(starts[k] + 2, blocks + 1) if k < len(starts) else blocks + 1
        return depth * last + LANES

    for k, first in enumerate(starts):
        width = depth * (min(first + 2, blocks + 1) - first)
        need = upto(k + 1)
        if need > built:
            build_hankel(record, hankel, built // LANES, need // LANES)
        built = need
        for b in range(first, first + width // depth):
            piece = None
            for c in range(chans):
                start = depth * b
                columns = jnp.concatenate([hankel[c, :, start + LANES * q : start + LANES * q + depth] for q in range(2)], axis=0)
                part = jnp.dot(stacked[c], columns, preferred_element_type=jnp.float32)
                piece = part if piece is None else piece + part
            if b:
                total = pending + piece[rows:] * factor
                corr[pl.ds(2 * b - 2, rows, stride=stride), :] = total[:, :LANES]
                corr[pl.ds(2 * b - 1, rows, stride=stride), :] = total[:, LANES:]
            pending = piece[:rows] * factor


FINE = 16


def deviation_scale(stack, groups, total):
    width = 512.0 / BINS
    count = stack.shape[0] // groups
    position = jnp.clip(jnp.abs(stack) / width - 0.5, 0.0, BINS - 1.0)
    lower = jnp.minimum(jnp.floor(position), BINS - 2.0)
    share = position - lower
    head = share.astype(jnp.bfloat16).astype(jnp.float32)
    tail = share - head
    coarse = jnp.floor(lower * (1.0 / FINE))
    fine = lower - FINE * coarse
    broad = lax.broadcasted_iota(jnp.int32, (BINS // FINE, LANES), 0).astype(jnp.float32)
    few = lax.broadcasted_iota(jnp.int32, (FINE, LANES), 0).astype(jnp.float32)
    row = lax.broadcasted_iota(jnp.int32, (FINE, LANES), 0)
    lane = lax.broadcasted_iota(jnp.int32, (FINE, LANES), 1)
    scales = []
    for t in range(groups):
        below, weights = [], []
        for r in range(t * count, (t + 1) * count):
            below.append((coarse[r : r + 1, :] <= broad).astype(jnp.float32).astype(jnp.bfloat16))
            upto = (fine[r : r + 1, :] <= few).astype(jnp.float32)
            same = fine[r : r + 1, :] == few
            parts = [upto, same.astype(jnp.float32), jnp.where(same, head[r : r + 1, :], 0.0), jnp.where(same, tail[r : r + 1, :], 0.0)]
            weights.append(jnp.concatenate(parts, axis=0).astype(jnp.bfloat16))
        weight = jnp.concatenate(weights, axis=1)
        below = jnp.concatenate(below, axis=1)
        found = lax.dot_general(weight, below, (((1,), (1,)), ((), ())), preferred_element_type=jnp.float32)
        if found.shape[1] < LANES:
            found = jnp.concatenate([found, jnp.zeros((found.shape[0], LANES - found.shape[1]), jnp.float32)], axis=1)
        upto, same = found[:FINE], found[FINE : 2 * FINE]
        part = found[2 * FINE : 3 * FINE] + found[3 * FINE :]
        upto_left = jnp.where(lane >= 1, pltpu.roll(upto, 1, 1), 0.0)
        same_left = jnp.where(lane >= 1, pltpu.roll(same, 1, 1), 0.0)
        part_left = jnp.where(lane >= 1, pltpu.roll(part, 1, 1), 0.0)
        part_far = jnp.where(lane >= 2, pltpu.roll(part, 2, 1), 0.0)
        held = same - same_left
        moved = part - part_left
        spilled = pltpu.roll(jnp.where(row == FINE - 1, part_left - part_far, moved), 1, 0)
        counts = held - moved + spilled
        prior = upto_left[FINE - 1 : FINE, :]
        earlier = prior + (upto - upto_left) - held - spilled
        portion = jnp.clip((0.5 * total - earlier) / jnp.maximum(counts, 1.0), 0.0, 1.0)
        portion = jnp.where(lane < BINS // FINE, portion, 0.0)
        portion = jnp.sum(portion, axis=0, keepdims=True)
        scales.append(1.4826 * (width * jnp.sum(portion, axis=1, keepdims=True)))
    return scales


LEVELS = 32600.0
ROUNDER = 12582912.0
CODE_STEP = 64.0


def encode(pieces, target, slot):
    half = len(pieces) // 2
    rows = pieces[0].shape[0]
    codes, inverses = [], []
    for group in (pieces[:half], pieces[half:]):
        most = jnp.abs(group[0])
        for piece in group[1:]:
            most = jnp.maximum(most, jnp.abs(piece))
        most = jnp.maximum(jnp.max(most, axis=0, keepdims=True), 1e-30)
        code = jnp.floor(jnp.log2(most) * CODE_STEP) + 1.0
        inverses.append(LEVELS * jnp.exp2(code * (-1.0 / CODE_STEP)))
        codes.append(code.astype(jnp.int32))
    for p in range(half):
        high = (pieces[p] * inverses[0] + ROUNDER).astype(jnp.int32)
        low = (pieces[p + half] * inverses[1] + ROUNDER).astype(jnp.int32)
        target[slot, p * rows : (p + 1) * rows, :] = (high << 16) | (low & 65535)
    target[slot, half * rows : half * rows + 1, :] = (codes[0] << 16) | (codes[1] & 65535)


def decode(source, slot, half, rows):
    def split(word):
        return (word >> 16).astype(jnp.float32), ((word << 16) >> 16).astype(jnp.float32)

    scales = [jnp.exp2(code * (1.0 / CODE_STEP)) * (1.0 / LEVELS) for code in split(source[slot, half * rows : half * rows + 1, :])]
    highs, lows = [], []
    for p in range(half):
        high, low = split(source[slot, p * rows : (p + 1) * rows, :])
        highs.append(high * scales[0])
        lows.append(low * scales[1])
    return highs + lows


def stack_kernel(n, m, own, blocks, stride, lags_hbm, present_hbm, wave_hbm, pattern_hbm, score_ref, scale_ref, peak_ref, out_ref, lags_ref, present_ref, wave_ref, pattern_ref, load_sem, record, hankel, corr, packed, recv1, scored, send2, recv2, send3, recv3, send_sem, recv1_sem, recv2_sem, recv3_sem):
    me, group = lax.axis_index("sta"), lax.axis_index("tpl")
    owners = n // 2
    quarter = n // 4
    half = send2.shape[1]
    groups = 2 * half
    rows = pattern_ref.shape[0]
    count = n * own // LANES
    chunk = groups * count
    upper = (me >= owners).astype(jnp.int32)
    virtual = upper * quarter + lax.rem(me, quarter)
    owner = jnp.logical_and(me >= quarter, me < 3 * quarter)
    outer = 1 - owner.astype(jnp.int32)

    def peer(d):
        return me ^ d

    def fellow(e):
        return lax.rem(group + e, m)

    loads = [
        pltpu.make_async_copy(source, target, load_sem.at[k])
        for k, (source, target) in enumerate(
            ((wave_hbm, wave_ref), (pattern_hbm, pattern_ref), (lags_hbm, lags_ref), (present_hbm, present_ref))
        )
    ]
    for load in loads:
        load.start()

    barrier = pltpu.get_barrier_semaphore()

    @pl.when(owner)
    def greet():
        for d in range(n - 1, 0, -1):
            pl.semaphore_signal(barrier, inc=1, device_id={"sta": peer(d), "tpl": group}, device_id_type=MESH)

    for e in range(1, m):
        pl.semaphore_signal(barrier, inc=1, device_id={"sta": me, "tpl": fellow(e)}, device_id_type=MESH)

    def move(source, target, send, recv, sta, tpl):
        return pltpu.make_async_remote_copy(
            src_ref=source,
            dst_ref=target,
            send_sem=send_sem.at[send],
            recv_sem=recv,
            device_id={"sta": sta, "tpl": tpl},
            device_id_type=MESH,
        )

    def copy1(k):
        band = 2 * outer + (1 if k >= quarter else 0)
        return move(packed.at[k], recv1.at[outer * owners + k], 0, recv1_sem.at[band], quarter + (virtual ^ k), group)

    def span1(low, high, band):
        part = recv1.at[pl.ds(low, high - low)]
        return move(part, part, 0, recv1_sem.at[band], peer(1), group)

    def copy2(p):
        return move(send2.at[p], recv2.at[virtual], 1, recv2_sem, p, group)

    def span2(size):
        part = recv2.at[pl.ds(0, size)]
        return move(part, part, 1, recv2_sem, peer(1), group)

    def copy3(e, p):
        return move(send3.at[p], recv3.at[e - 1, virtual], 2, recv3_sem, p, fellow(e))

    loads[0].wait()
    correlate(blocks, stride, wave_ref, pattern_ref, record, hankel, corr, loads[1])

    loads[2].wait()
    loads[3].wait()
    lane = lax.broadcasted_iota(jnp.int32, (count, LANES), 1)

    def shifted(k):
        found = []
        for p in range(groups):
            t = (p // half) * (rows // 2) + (virtual ^ k) * half + p % half
            lag = lags_ref[t]
            begin = t * stride + (lag >> 7)
            rest = lag & (LANES - 1)
            near = corr[pl.ds(begin, count), :]
            after = corr[pl.ds(begin + 1, count), :]
            joined = pltpu.roll(jnp.where(lane >= rest, near, after), (LANES - rest) & (LANES - 1), 1)
            found.append(joined * present_ref[t].astype(jnp.float32))
        return found

    order = sorted(range(1, owners), key=lambda k: (-(k & (quarter // 2)), -k))
    encode(shifted(order[0]), packed, order[0])
    pl.semaphore_wait(barrier, owners + m - 2 + outer)
    copy1(order[0]).start()
    begin, size = 1, 3
    while begin < len(order):
        batch = order[begin : begin + size]
        for k in batch:
            encode(shifted(k), packed, k)
        for k in batch:
            copy1(k).start()
        begin += size

    @pl.when(jnp.logical_not(owner))
    def last():
        encode(shifted(0), packed, 0)
        copy1(0).start()

    @pl.when(owner)
    def serve():
        total = shifted(0)
        for band, low, high in ((0, 1, quarter), (1, quarter, owners), (2, owners, owners + quarter), (3, owners + quarter, n)):
            span1(low, high, band).wait_recv()
            for slot in range(low, high):
                total = [a + b for a, b in zip(total, decode(recv1, slot, half, count))]
        for p in range(groups):
            scored[p * count : (p + 1) * count, :] = total[p]
        scored[chunk:, :] = jnp.zeros((8, LANES), jnp.float32)
        stack = scored[:chunk, :]
        lane = lax.broadcasted_iota(jnp.int32, (half, LANES), 1)
        middle = LANES // 2
        views = []
        for j in range(n):
            begin, rest = divmod(own * j, LANES)
            sides = []
            for side in range(2):
                first = side * half * count + begin
                near = scored[pl.ds(first, half, stride=count), :]
                if rest:
                    after = scored[pl.ds(first + 1, half, stride=count), :]
                    near = jnp.where(lane >= rest, near, after)
                turn = (side * middle - rest) % LANES
                sides.append(pltpu.roll(near, turn, 1) if turn else near)
            views.append(jnp.where(lane < middle, sides[0], sides[1]))
        scales = deviation_scale(stack, groups, n * own)
        scale = jnp.where(lane < middle, jnp.concatenate(scales[:half], axis=0), jnp.concatenate(scales[half:], axis=0))
        inverse = 1.0 / scale

        def ready(targets):
            for j in targets:
                near = views[j] * inverse
                send2[j] = jnp.where((lane & (middle - 1)) < own, near, scale)
                send3[j] = jnp.max(near, axis=0, keepdims=True)

        def leave(targets):
            for p in targets:
                if m == 2:
                    copy3(1, p).start()
                if quarter <= p < 3 * quarter:

                    @pl.when(me != p)
                    def start2():
                        copy2(p).start()

                else:
                    copy2(p).start()

        ready(range(quarter))
        leave(range(quarter))
        ready(range(quarter, n))
        leave(range(quarter, n))
        if m > 2:
            for e in range(1, m):

                def start3(p, carry):
                    copy3(e, p).start()
                    return carry

                lax.fori_loop(0, n, start3, 0)
        recv2[virtual] = send2[me]

    @pl.when(owner)
    def arrive_owner():
        span2(owners - 1).wait_recv()

    @pl.when(jnp.logical_not(owner))
    def arrive():
        span2(owners).wait_recv()

    top = recv2[0]
    for i in range(owners):
        piece = recv2[i]
        out_ref[i * half : (i + 1) * half, :] = piece
        top = jnp.maximum(top, piece)
    out_ref[rows // 2 :, :] = pltpu.roll(out_ref[: rows // 2, :], LANES // 2, 1)
    top = jnp.max(top, axis=0, keepdims=True)
    turned = out_ref[...].T
    score_ref[...] = turned[:own, :]
    scale_ref[...] = turned[own, :]
    if m > 1:
        move(recv3, recv3, 2, recv3_sem, peer(1), group).wait_recv()
        for e in range(m - 1):
            top = jnp.maximum(top, jnp.max(recv3[e], axis=0))
    top = jnp.maximum(top, pltpu.roll(top, LANES // 2, 1))
    peak_ref[...] = top[0, :own]

    @pl.when(jnp.logical_not(owner))
    def drain():
        span1(0, owners, 0).wait_send()

    @pl.when(owner)
    def drain_owner():
        span1(1, owners, 0).wait_send()
        move(send2.at[pl.ds(0, n - 1)], send2.at[pl.ds(0, n - 1)], 1, recv2_sem, peer(1), group).wait_send()
        for e in range(1, m):
            move(send3, send3, 2, recv3_sem, peer(1), group).wait_send()


def stack_and_score(wave, pattern, lags, present, n, m):
    chans, samples = wave.shape
    rows = pattern.shape[0]
    total = TOUT_DEV * n
    blocks = -(-(total + LAG) // (2 * LANES))
    span = 2 * LANES * (blocks + 1) + LANES
    padded = ceil_to(max(span + LANES, samples), LANES)
    count = total // LANES
    stride = max(2 * blocks, LAG // LANES + count + 2) | 1
    owners = n // 2
    groups = rows // owners
    chunk = groups * count
    words = chunk // 2 + 1
    vmem = pl.BlockSpec(memory_space=pltpu.VMEM)
    return pl.pallas_call(
        functools.partial(stack_kernel, n, m, TOUT_DEV, blocks, stride),
        out_shape=(pltpu.VMEM((TOUT_DEV, rows), jnp.float32), pltpu.VMEM((rows,), jnp.float32), pltpu.VMEM((TOUT_DEV,), jnp.float32)),
        in_specs=[pl.BlockSpec(memory_space=pltpu.HBM)] * 4,
        out_specs=(vmem, vmem, vmem),
        scratch_shapes=[
            pltpu.VMEM((rows, LANES), jnp.float32),
            pltpu.SMEM(lags.shape, lags.dtype),
            pltpu.SMEM(present.shape, present.dtype),
            pltpu.VMEM(wave.shape, wave.dtype),
            pltpu.VMEM(pattern.shape, pattern.dtype),
            pltpu.SemaphoreType.DMA((4,)),
            pltpu.VMEM((chans, padded), jnp.float32),
            pltpu.VMEM((chans, LANES, span), jnp.bfloat16),
            pltpu.VMEM((rows * stride, LANES), jnp.float32),
            pltpu.VMEM((owners, words, LANES), jnp.int32),
            pltpu.VMEM((n, words, LANES), jnp.int32),
            pltpu.VMEM((chunk + 8, LANES), jnp.float32),
            pltpu.VMEM((n, groups // 2, LANES), jnp.float32),
            pltpu.VMEM((owners, groups // 2, LANES), jnp.float32),
            pltpu.VMEM((n, 1, LANES), jnp.float32),
            pltpu.VMEM((max(m - 1, 1), owners, 1, LANES), jnp.float32),
            pltpu.SemaphoreType.DMA((3,)),
            pltpu.SemaphoreType.DMA((4,)),
            pltpu.SemaphoreType.DMA,
            pltpu.SemaphoreType.DMA,
        ],
        compiler_params=pltpu.CompilerParams(collective_id=0, has_side_effects=True),
    )(lags, present, wave, pattern)


def finish_kernel(score, scale, peak, score_out, scale_out, peak_out, sems):
    pairs = ((score, score_out), (scale, scale_out), (peak, peak_out))
    copies = [pltpu.make_async_copy(source, target, sems.at[k]) for k, (source, target) in enumerate(pairs)]
    for copy in copies:
        copy.start()
    for copy in copies:
        copy.wait()


def on_device(waveform, templates, lags, present):
    n, m = lax.axis_size("sta"), lax.axis_size("tpl")
    found = stack_and_score(waveform[0], templates[:, 0, :], lags[:, 0], present[:, 0], n, m)
    return pl.pallas_call(
        finish_kernel,
        out_shape=tuple(jax.ShapeDtypeStruct(part.shape, part.dtype) for part in found),
        in_specs=[pl.BlockSpec(memory_space=pltpu.VMEM)] * 3,
        out_specs=(pl.BlockSpec(memory_space=pltpu.HBM),) * 3,
        scratch_shapes=[pltpu.SemaphoreType.DMA((3,))],
        compiler_params=pltpu.CompilerParams(vmem_limit_bytes=VMEM_LIMIT),
    )(*found)


def solution(mesh):
    placed = (P("sta", None, None), P("tpl", "sta", None), P("tpl", "sta"), P("tpl", "sta"))
    return jax.shard_map(
        on_device,
        mesh=mesh,
        in_specs=placed,
        out_specs=(P("sta", "tpl"), P("tpl"), P("sta")),
        check_vma=False,
    )
```

```python
import functools

import jax
import jax.numpy as jnp
from jax import lax
from jax.experimental import pallas as pl
from jax.experimental.pallas import tpu as pltpu
from jax.sharding import PartitionSpec as P

LEN = 512
LAG = 3000
BINS = 1024
TOUT_DEV = 48
LANES = 128
VMEM_LIMIT = 16 * 1024 * 1024
MESH = pl.DeviceIdType.MESH


def ceil_to(value, step):
    return -(-value // step) * step


def build_hankel(record, hankel, first, last):
    row = lax.broadcasted_iota(jnp.int32, (16, LANES), 0)
    back = (lax.broadcasted_iota(jnp.int32, (16, LANES), 1) + row - 2 * (row & 7)).astype(jnp.float32).astype(jnp.bfloat16)
    back = jnp.concatenate([back] * (last - first), axis=1)

    def turned(c, j, a):
        line = jnp.broadcast_to(record[c : c + 1, j * LANES : (j + 1) * LANES], (8, LANES))
        return pltpu.roll(line, LANES - 7 - 8 * a, 1, stride=1, stride_axis=0)

    for c in range(hankel.shape[0]):
        for g in range(LANES // 16):
            halves = [jnp.concatenate([turned(c, j, a) for j in range(first, last + 1)], axis=1) for a in (2 * g, 2 * g + 1)]
            both = jnp.concatenate(halves, axis=0).astype(jnp.bfloat16)
            hankel[c, 16 * g : 16 * g + 16, first * LANES : last * LANES] = jnp.where(
                back < float(LANES - 7 - 16 * g), both[:, :-LANES], both[:, LANES:]
            )


def reverse_eights(pattern):
    rows, width = pattern.shape
    source = lax.broadcasted_iota(jnp.int32, (LANES, LANES), 0)
    target = lax.broadcasted_iota(jnp.int32, (LANES, LANES), 1)
    swap = (source == (target ^ 7)).astype(jnp.float32).astype(jnp.bfloat16)
    chunks = jnp.concatenate([pattern[:, k * LANES : (k + 1) * LANES] for k in range(width // LANES)], axis=0)
    turned = jnp.dot(chunks, swap, preferred_element_type=jnp.float32).astype(jnp.bfloat16)
    return [turned[k * rows : (k + 1) * rows] for k in range(width // LANES)]


def correlate(blocks, stride, wave_ref, pattern_ref, record, hankel, corr, load):
    chans, samples = wave_ref.shape
    rows = pattern_ref.shape[0]
    span = hankel.shape[2]
    record[...] = jnp.zeros_like(record)
    record[:, :samples] = wave_ref[...].astype(jnp.float32)
    depth = 2 * LANES
    built = depth * min(4, blocks + 1) + LANES
    build_hankel(record, hankel, 0, built // LANES)
    load.wait()
    pattern = pattern_ref[...]
    wide = pattern.astype(jnp.float32)
    factor = 1.0 / jnp.sqrt(jnp.sum(wide * wide, axis=1, keepdims=True) + 1e-06)
    chunks = reverse_eights(pattern)
    per = LEN // LANES
    stacked = []
    for c in range(chans):
        halves = [jnp.concatenate([chunks[c * per + 2 * h + q] for q in range(2)], axis=1) for h in range(LEN // depth)]
        stacked.append(jnp.concatenate(halves, axis=0))
    starts = list(range(0, blocks + 1, 2))
    pending = None

    def upto(k):
        last = min(starts[k] + 2, blocks + 1) if k < len(starts) else blocks + 1
        return depth * last + LANES

    for k, first in enumerate(starts):
        width = depth * (min(first + 2, blocks + 1) - first)
        need = upto(k + 1)
        if need > built:
            build_hankel(record, hankel, built // LANES, need // LANES)
        built = need
        for b in range(first, first + width // depth):
            piece = None
            for c in range(chans):
                start = depth * b
                columns = jnp.concatenate([hankel[c, :, start + LANES * q : start + LANES * q + depth] for q in range(2)], axis=0)
                part = jnp.dot(stacked[c], columns, preferred_element_type=jnp.float32)
                piece = part if piece is None else piece + part
            if b:
                total = pending + piece[rows:] * factor
                corr[pl.ds(2 * b - 2, rows, stride=stride), :] = total[:, :LANES]
                corr[pl.ds(2 * b - 1, rows, stride=stride), :] = total[:, LANES:]
            pending = piece[:rows] * factor


FINE = 16


def deviation_scale(stack, groups, total):
    width = 512.0 / BINS
    count = stack.shape[0] // groups
    position = jnp.clip(jnp.abs(stack) / width - 0.5, 0.0, BINS - 1.0)
    lower = jnp.minimum(jnp.floor(position), BINS - 2.0)
    share = position - lower
    head = share.astype(jnp.bfloat16).astype(jnp.float32)
    tail = share - head
    coarse = jnp.floor(lower * (1.0 / FINE))
    fine = lower - FINE * coarse
    broad = lax.broadcasted_iota(jnp.int32, (BINS // FINE, LANES), 0).astype(jnp.float32)
    few = lax.broadcasted_iota(jnp.int32, (FINE, LANES), 0).astype(jnp.float32)
    row = lax.broadcasted_iota(jnp.int32, (FINE, LANES), 0)
    lane = lax.broadcasted_iota(jnp.int32, (FINE, LANES), 1)
    scales = []
    for t in range(groups):
        below, weights = [], []
        for r in range(t * count, (t + 1) * count):
            below.append((coarse[r : r + 1, :] <= broad).astype(jnp.float32).astype(jnp.bfloat16))
            upto = (fine[r : r + 1, :] <= few).astype(jnp.float32)
            same = fine[r : r + 1, :] == few
            parts = [upto, same.astype(jnp.float32), jnp.where(same, head[r : r + 1, :], 0.0), jnp.where(same, tail[r : r + 1, :], 0.0)]
            weights.append(jnp.concatenate(parts, axis=0).astype(jnp.bfloat16))
        weight = jnp.concatenate(weights, axis=1)
        below = jnp.concatenate(below, axis=1)
        found = lax.dot_general(weight, below, (((1,), (1,)), ((), ())), preferred_element_type=jnp.float32)
        if found.shape[1] < LANES:
            found = jnp.concatenate([found, jnp.zeros((found.shape[0], LANES - found.shape[1]), jnp.float32)], axis=1)
        upto, same = found[:FINE], found[FINE : 2 * FINE]
        part = found[2 * FINE : 3 * FINE] + found[3 * FINE :]
        upto_left = jnp.where(lane >= 1, pltpu.roll(upto, 1, 1), 0.0)
        same_left = jnp.where(lane >= 1, pltpu.roll(same, 1, 1), 0.0)
        part_left = jnp.where(lane >= 1, pltpu.roll(part, 1, 1), 0.0)
        part_far = jnp.where(lane >= 2, pltpu.roll(part, 2, 1), 0.0)
        held = same - same_left
        moved = part - part_left
        spilled = pltpu.roll(jnp.where(row == FINE - 1, part_left - part_far, moved), 1, 0)
        counts = held - moved + spilled
        prior = upto_left[FINE - 1 : FINE, :]
        earlier = prior + (upto - upto_left) - held - spilled
        portion = jnp.clip((0.5 * total - earlier) / jnp.maximum(counts, 1.0), 0.0, 1.0)
        portion = jnp.where(lane < BINS // FINE, portion, 0.0)
        portion = jnp.sum(portion, axis=0, keepdims=True)
        scales.append(1.4826 * (width * jnp.sum(portion, axis=1, keepdims=True)))
    return scales


LEVELS = 32600.0
ROUNDER = 12582912.0
CODE_STEP = 64.0


def encode(pieces, target, slot):
    half = len(pieces) // 2
    rows = pieces[0].shape[0]
    codes, inverses = [], []
    for group in (pieces[:half], pieces[half:]):
        most = jnp.abs(group[0])
        for piece in group[1:]:
            most = jnp.maximum(most, jnp.abs(piece))
        most = jnp.maximum(jnp.max(most, axis=0, keepdims=True), 1e-30)
        code = jnp.floor(jnp.log2(most) * CODE_STEP) + 1.0
        inverses.append(LEVELS * jnp.exp2(code * (-1.0 / CODE_STEP)))
        codes.append(code.astype(jnp.int32))
    for p in range(half):
        high = (pieces[p] * inverses[0] + ROUNDER).astype(jnp.int32)
        low = (pieces[p + half] * inverses[1] + ROUNDER).astype(jnp.int32)
        target[slot, p * rows : (p + 1) * rows, :] = (high << 16) | (low & 65535)
    target[slot, half * rows : half * rows + 1, :] = (codes[0] << 16) | (codes[1] & 65535)


def decode(source, slot, half, rows):
    def split(word):
        return (word >> 16).astype(jnp.float32), ((word << 16) >> 16).astype(jnp.float32)

    scales = [jnp.exp2(code * (1.0 / CODE_STEP)) * (1.0 / LEVELS) for code in split(source[slot, half * rows : half * rows + 1, :])]
    highs, lows = [], []
    for p in range(half):
        high, low = split(source[slot, p * rows : (p + 1) * rows, :])
        highs.append(high * scales[0])
        lows.append(low * scales[1])
    return highs + lows


def stack_kernel(n, m, own, blocks, stride, lags_hbm, present_hbm, wave_hbm, pattern_hbm, score_ref, scale_ref, peak_ref, out_ref, lags_ref, present_ref, wave_ref, pattern_ref, load_sem, record, hankel, corr, packed, recv1, scored, send2, recv2, send3, recv3, send_sem, recv1_sem, recv2_sem, recv3_sem):
    me, group = lax.axis_index("sta"), lax.axis_index("tpl")
    owners = n // 2
    quarter = n // 4
    half = send2.shape[1]
    groups = 2 * half
    rows = pattern_ref.shape[0]
    count = n * own // LANES
    chunk = groups * count
    upper = (me >= owners).astype(jnp.int32)
    virtual = upper * quarter + lax.rem(me, quarter)
    owner = jnp.logical_and(me >= quarter, me < 3 * quarter)
    outer = 1 - owner.astype(jnp.int32)

    def peer(d):
        return me ^ d

    def fellow(e):
        return lax.rem(group + e, m)

    loads = [
        pltpu.make_async_copy(source, target, load_sem.at[k])
        for k, (source, target) in enumerate(
            ((wave_hbm, wave_ref), (pattern_hbm, pattern_ref), (lags_hbm, lags_ref), (present_hbm, present_ref))
        )
    ]
    for load in loads:
        load.start()

    barrier = pltpu.get_barrier_semaphore()

    @pl.when(owner)
    def greet():
        for d in range(n - 1, 0, -1):
            pl.semaphore_signal(barrier, inc=1, device_id={"sta": peer(d), "tpl": group}, device_id_type=MESH)

    for e in range(1, m):
        pl.semaphore_signal(barrier, inc=1, device_id={"sta": me, "tpl": fellow(e)}, device_id_type=MESH)

    def move(source, target, send, recv, sta, tpl):
        return pltpu.make_async_remote_copy(
            src_ref=source,
            dst_ref=target,
            send_sem=send_sem.at[send],
            recv_sem=recv,
            device_id={"sta": sta, "tpl": tpl},
            device_id_type=MESH,
        )

    def copy1(k):
        band = 2 * outer + (1 if k >= quarter else 0)
        return move(packed.at[k], recv1.at[outer * owners + k], 0, recv1_sem.at[band], quarter + (virtual ^ k), group)

    def span1(low, high, band):
        part = recv1.at[pl.ds(low, high - low)]
        return move(part, part, 0, recv1_sem.at[band], peer(1), group)

    def copy2(p):
        return move(send2.at[p], recv2.at[virtual], 1, recv2_sem, p, group)

    def span2(size):
        part = recv2.at[pl.ds(0, size)]
        return move(part, part, 1, recv2_sem, peer(1), group)

    def copy3(e, p):
        return move(send3.at[p], recv3.at[e - 1, virtual], 2, recv3_sem, p, fellow(e))

    loads[0].wait()
    correlate(blocks, stride, wave_ref, pattern_ref, record, hankel, corr, loads[1])

    loads[2].wait()
    loads[3].wait()
    lane = lax.broadcasted_iota(jnp.int32, (count, LANES), 1)

    def shifted(k):
        found = []
        for p in range(groups):
            t = (p // half) * (rows // 2) + (virtual ^ k) * half + p % half
            lag = lags_ref[t]
            begin = t * stride + (lag >> 7)
            rest = lag & (LANES - 1)
            near = corr[pl.ds(begin, count), :]
            after = corr[pl.ds(begin + 1, count), :]
            joined = pltpu.roll(jnp.where(lane >= rest, near, after), (LANES - rest) & (LANES - 1), 1)
            found.append(joined * present_ref[t].astype(jnp.float32))
        return found

    order = sorted(range(1, owners), key=lambda k: (-(k & (quarter // 2)), -k))
    encode(shifted(order[0]), packed, order[0])
    pl.semaphore_wait(barrier, owners + m - 2 + outer)
    copy1(order[0]).start()
    begin, size = 1, 3
    while begin < len(order):
        batch = order[begin : begin + size]
        for k in batch:
            encode(shifted(k), packed, k)
        for k in batch:
            copy1(k).start()
        begin += size

    @pl.when(jnp.logical_not(owner))
    def last():
        encode(shifted(0), packed, 0)
        copy1(0).start()

    @pl.when(owner)
    def serve():
        total = shifted(0)
        sides = (owners + quarter * upper, owners + quarter * (1 - upper))
        for band, low, size in ((0, 1, quarter - 1), (1, quarter, quarter), (2 + upper, sides[0], quarter), (3 - upper, sides[1], quarter)):
            span1(1, size + 1, band).wait_recv()
            for slot in range(size):
                total = [a + b for a, b in zip(total, decode(recv1, low + slot, half, count))]
        for p in range(groups):
            scored[p * count : (p + 1) * count, :] = total[p]
        scored[chunk:, :] = jnp.zeros((8, LANES), jnp.float32)
        stack = scored[:chunk, :]
        lane = lax.broadcasted_iota(jnp.int32, (half, LANES), 1)
        middle = LANES // 2
        views = []
        for j in range(n):
            begin, rest = divmod(own * j, LANES)
            sides = []
            for side in range(2):
                first = side * half * count + begin
                near = scored[pl.ds(first, half, stride=count), :]
                if rest:
                    after = scored[pl.ds(first + 1, half, stride=count), :]
                    near = jnp.where(lane >= rest, near, after)
                turn = (side * middle - rest) % LANES
                sides.append(pltpu.roll(near, turn, 1) if turn else near)
            views.append(jnp.where(lane < middle, sides[0], sides[1]))
        scales = deviation_scale(stack, groups, n * own)
        scale = jnp.where(lane < middle, jnp.concatenate(scales[:half], axis=0), jnp.concatenate(scales[half:], axis=0))
        inverse = 1.0 / scale

        def ready(targets):
            for j in targets:
                near = views[j] * inverse
                send2[j] = jnp.where((lane & (middle - 1)) < own, near, scale)
                send3[j] = jnp.max(near, axis=0, keepdims=True)

        def leave(targets):
            for p in targets:
                if m == 2:
                    copy3(1, p).start()
                if quarter <= p < 3 * quarter:

                    @pl.when(me != p)
                    def start2():
                        copy2(p).start()

                else:
                    copy2(p).start()

        ready(range(quarter))
        leave(range(quarter))
        ready(range(quarter, n))
        leave(range(quarter, n))
        if m > 2:
            for e in range(1, m):

                def start3(p, carry):
                    copy3(e, p).start()
                    return carry

                lax.fori_loop(0, n, start3, 0)
        recv2[virtual] = send2[me]

    @pl.when(owner)
    def arrive_owner():
        span2(owners - 1).wait_recv()

    @pl.when(jnp.logical_not(owner))
    def arrive():
        span2(owners).wait_recv()

    top = recv2[0]
    for i in range(owners):
        piece = recv2[i]
        out_ref[i * half : (i + 1) * half, :] = piece
        top = jnp.maximum(top, piece)
    out_ref[rows // 2 :, :] = pltpu.roll(out_ref[: rows // 2, :], LANES // 2, 1)
    top = jnp.max(top, axis=0, keepdims=True)
    turned = out_ref[...].T
    score_ref[...] = turned[:own, :]
    scale_ref[...] = turned[own, :]
    if m > 1:
        move(recv3, recv3, 2, recv3_sem, peer(1), group).wait_recv()
        for e in range(m - 1):
            top = jnp.maximum(top, jnp.max(recv3[e], axis=0))
    top = jnp.maximum(top, pltpu.roll(top, LANES // 2, 1))
    peak_ref[...] = top[0, :own]

    @pl.when(jnp.logical_not(owner))
    def drain():
        span1(0, owners, 0).wait_send()

    @pl.when(owner)
    def drain_owner():
        span1(1, owners, 0).wait_send()
        move(send2.at[pl.ds(0, n - 1)], send2.at[pl.ds(0, n - 1)], 1, recv2_sem, peer(1), group).wait_send()
        for e in range(1, m):
            move(send3, send3, 2, recv3_sem, peer(1), group).wait_send()


def stack_and_score(wave, pattern, lags, present, n, m):
    chans, samples = wave.shape
    rows = pattern.shape[0]
    total = TOUT_DEV * n
    blocks = -(-(total + LAG) // (2 * LANES))
    span = 2 * LANES * (blocks + 1) + LANES
    padded = ceil_to(max(span + LANES, samples), LANES)
    count = total // LANES
    stride = max(2 * blocks, LAG // LANES + count + 2) | 1
    owners = n // 2
    groups = rows // owners
    chunk = groups * count
    words = chunk // 2 + 1
    vmem = pl.BlockSpec(memory_space=pltpu.VMEM)
    return pl.pallas_call(
        functools.partial(stack_kernel, n, m, TOUT_DEV, blocks, stride),
        out_shape=(pltpu.VMEM((TOUT_DEV, rows), jnp.float32), pltpu.VMEM((rows,), jnp.float32), pltpu.VMEM((TOUT_DEV,), jnp.float32)),
        in_specs=[pl.BlockSpec(memory_space=pltpu.HBM)] * 4,
        out_specs=(vmem, vmem, vmem),
        scratch_shapes=[
            pltpu.VMEM((rows, LANES), jnp.float32),
            pltpu.SMEM(lags.shape, lags.dtype),
            pltpu.SMEM(present.shape, present.dtype),
            pltpu.VMEM(wave.shape, wave.dtype),
            pltpu.VMEM(pattern.shape, pattern.dtype),
            pltpu.SemaphoreType.DMA((4,)),
            pltpu.VMEM((chans, padded), jnp.float32),
            pltpu.VMEM((chans, LANES, span), jnp.bfloat16),
            pltpu.VMEM((rows * stride, LANES), jnp.float32),
            pltpu.VMEM((owners, words, LANES), jnp.int32),
            pltpu.VMEM((n, words, LANES), jnp.int32),
            pltpu.VMEM((chunk + 8, LANES), jnp.float32),
            pltpu.VMEM((n, groups // 2, LANES), jnp.float32),
            pltpu.VMEM((owners, groups // 2, LANES), jnp.float32),
            pltpu.VMEM((n, 1, LANES), jnp.float32),
            pltpu.VMEM((max(m - 1, 1), owners, 1, LANES), jnp.float32),
            pltpu.SemaphoreType.DMA((3,)),
            pltpu.SemaphoreType.DMA((4,)),
            pltpu.SemaphoreType.DMA,
            pltpu.SemaphoreType.DMA,
        ],
        compiler_params=pltpu.CompilerParams(collective_id=0, has_side_effects=True),
    )(lags, present, wave, pattern)


def finish_kernel(score, scale, peak, score_out, scale_out, peak_out, sems):
    pairs = ((score, score_out), (scale, scale_out), (peak, peak_out))
    copies = [pltpu.make_async_copy(source, target, sems.at[k]) for k, (source, target) in enumerate(pairs)]
    for copy in copies:
        copy.start()
    for copy in copies:
        copy.wait()


def on_device(waveform, templates, lags, present):
    n, m = lax.axis_size("sta"), lax.axis_size("tpl")
    found = stack_and_score(waveform[0], templates[:, 0, :], lags[:, 0], present[:, 0], n, m)
    return pl.pallas_call(
        finish_kernel,
        out_shape=tuple(jax.ShapeDtypeStruct(part.shape, part.dtype) for part in found),
        in_specs=[pl.BlockSpec(memory_space=pltpu.VMEM)] * 3,
        out_specs=(pl.BlockSpec(memory_space=pltpu.HBM),) * 3,
        scratch_shapes=[pltpu.SemaphoreType.DMA((3,))],
        compiler_params=pltpu.CompilerParams(vmem_limit_bytes=VMEM_LIMIT),
    )(*found)


def solution(mesh):
    placed = (P("sta", None, None), P("tpl", "sta", None), P("tpl", "sta"), P("tpl", "sta"))
    return jax.shard_map(
        on_device,
        mesh=mesh,
        in_specs=placed,
        out_specs=(P("sta", "tpl"), P("tpl"), P("sta")),
        check_vma=False,
    )
```
